128 devices in a mesh: groups: 4 (over x, y), blk: 32 (over z, core).
Axes of the slice: x: 2, y: 2, z: 16, core: 2. Of those that a mesh axis runs over, the one named last changes fastest.
The devices are a block of a 8x8x16 slice.
Arguments:
- coords: float32 [32, 98304], P(None, ('groups', 'blk')), parts along dimension 1, may hold values from -6 to 6
- alpha: float32 [98304], P(('groups', 'blk')), parts along dimension 0, may hold values from -6 to 6
- probe_solves: float32 [15, 98304], P(None, ('groups', 'blk')), parts along dimension 1, may hold values from -6 to 6
- probes: float32 [15, 98304], P(None, ('groups', 'blk')), parts along dimension 1, may hold values from -6 to 6
- lengthscale: float32 [32], replicated, may hold values from 4 to 12
Outputs:
- grad: float32 [32, 98304], P(None, ('groups', 'blk')), parts along dimension 1
The draws below stay inside these ranges and needn't reach their ends.
There are 4 independent parts, one for each index of `groups`. The reference program is written for one: setup_inputs(seed, part) draws one part's arguments, and reference() takes and returns one part's arrays. A program takes and returns all parts, laid end to end along the dimension named above; an argument that names none is the same for every part. Nothing has to cross between parts.
All inputs are finite; a program needn't handle non-finite values.
Results may differ from the reference program's by a relative error of at most 0.00014.
Values sent between devices are 32-bit elements; how exact they have to be, the bound alone decides.
A program may use at most 64 MiB of HBM per device.

```python
import math
import jax
import jax.numpy as jnp
from jax import lax

DIM = 32
PROBES = 15
BLOCK = 768
STEPS = 8
NPTS = 24576
N_BLK = 32


def levels(own_key, extent, shards, least, largest):
    level, own = 1.0, jax.random.fold_in(own_key, 6)
    for dim, blocks in shards:
        heights = jnp.exp(jax.random.uniform(jax.random.fold_in(own, dim), (blocks,), jnp.float32, least / len(shards), largest / len(shards)))
        level = level * jnp.repeat(heights, extent[dim] // blocks).reshape([-1 if axis == dim else 1 for axis in range(len(extent))])
    return level


def scatter_about(key, dims, deviation, most, split=(), dtype=jnp.bfloat16):
    drawn = deviation * jax.random.normal(key, dims, jnp.float32)
    if split:
        drawn = drawn * levels(key, dims, split, -0.22, 0.18)
    return jnp.clip(drawn, -most, most).astype(dtype)


def setup_inputs(seed: int = 0, part: int = 0) -> dict:
    seeds = jax.random.split(jax.random.key(seed), 6)
    part_splits = jax.random.split(jax.random.fold_in(seeds[5], part), 6)
    return {
        "coords": scatter_about(part_splits[0], (DIM, NPTS), 1.0, 6.0, ((1, 32),), jnp.float32),
        "alpha": scatter_about(part_splits[1], (NPTS,), 1.0, 6.0, ((0, 32),), jnp.float32),
        "probe_solves": scatter_about(part_splits[2], (PROBES, NPTS), 1.0, 6.0, ((1, 32),), jnp.float32),
        "probes": scatter_about(part_splits[3], (PROBES, NPTS), 1.0, 6.0, ((1, 32),), jnp.float32),
        "lengthscale": jnp.clip(jnp.exp(jax.random.uniform(seeds[4], (DIM,), jnp.float32, math.log(4.0), math.log(12.0))), 4.0, 12.0),
    }


root_five = 5.0 ** 0.5

def tile_terms(own_scaled, own_table, vis_scaled, vis_table):
    probe_count = (own_table.shape[0] - 1) // 2
    half_inv = 1.0 / (2.0 * probe_count)
    left_rows = jnp.concatenate([own_table[:1], -half_inv * own_table[1:]], 0)
    right_rows = jnp.concatenate([vis_table[:1], vis_table[1 + probe_count:], vis_table[1:1 + probe_count]], 0)
    contract_first = (((0,), (0,)), ((), ()))
    inner = lax.dot_general(own_scaled, vis_scaled, contract_first, precision=lax.Precision.HIGHEST, preferred_element_type=jnp.float32)
    own_square = lax.optimization_barrier(jnp.sum(own_scaled * own_scaled, 0))
    vis_square = lax.optimization_barrier(jnp.sum(vis_scaled * vis_scaled, 0))
    distance = own_square[:, None] + vis_square[None, :] - 2.0 * inner
    radius = jnp.sqrt(jnp.maximum(distance, 0.0))
    profile = (1.0 + root_five * radius) * jnp.exp(-root_five * radius)
    coupling = lax.dot_general(left_rows, right_rows, contract_first, precision=lax.Precision.HIGHEST, preferred_element_type=jnp.float32)
    weighted = coupling * profile
    row_part = own_scaled * lax.optimization_barrier(jnp.sum(weighted, 1))[None, :] - lax.dot_general(vis_scaled, weighted, (((1,), (1,)), ((), ())), precision=lax.Precision.HIGHEST, preferred_element_type=jnp.float32)
    col_part = vis_scaled * lax.optimization_barrier(jnp.sum(weighted, 0))[None, :] - jnp.dot(own_scaled, weighted, precision=lax.Precision.HIGHEST, preferred_element_type=jnp.float32)
    return (row_part, col_part)

def reference(coords, alpha, probe_solves, probes, lengthscale):
    scaled = coords / lengthscale[:, None]
    table = jnp.concatenate([alpha[None], probe_solves, probes], 0)
    blocks_scaled = scaled.reshape(DIM, N_BLK, BLOCK).transpose(1, 0, 2)
    blocks_table = table.reshape(table.shape[0], N_BLK, BLOCK).transpose(1, 0, 2)
    row_total = jnp.zeros(blocks_scaled.shape, jnp.float32)
    col_total = jnp.zeros(blocks_scaled.shape, jnp.float32)
    for offset in range(1, STEPS + 1):
        vis_scaled = jnp.roll(blocks_scaled, -offset, axis=0)
        vis_table = jnp.roll(blocks_table, -offset, axis=0)
        rows_now, cols_now = lax.map(lambda pieces: tile_terms(pieces[0], pieces[1], pieces[2], pieces[3]), (blocks_scaled, blocks_table, vis_scaled, vis_table))
        row_total = row_total + rows_now
        col_total = col_total + jnp.roll(cols_now, offset, axis=0)
    summed = (row_total + col_total).transpose(1, 0, 2).reshape(DIM, N_BLK * BLOCK)
    return -(5.0 / 3.0) / lengthscale[:, None] * summed
```

```python
import functools
import math

import jax
import jax.numpy as jnp
from jax import lax
from jax.experimental import pallas as pl
from jax.experimental.pallas import tpu as pltpu
from jax.sharding import PartitionSpec as P

F32 = jnp.float32
BF16 = jnp.bfloat16
MESH = pl.DeviceIdType.MESH

UNIT = math.sqrt(5.0) * math.log2(math.e)
LN2 = math.log(2.0)

CHUNK = 256
DEPTH = 208
OWN, PARTNER, UP, DOWN, P_UP, P_DOWN, SLOTS = 0, 1, 2, 6, 10, 14, 18


def split3(x):
    hi = x.astype(BF16)
    rest = x - hi.astype(F32)
    mid = rest.astype(BF16)
    lo = (rest - mid.astype(F32)).astype(BF16)
    return hi, mid, lo


def split2(x):
    hi = x.astype(BF16)
    return hi, (x - hi.astype(F32)).astype(BF16)


def column_of(row, dim):
    sub = lax.broadcasted_iota(jnp.int32, (dim, dim), 0)
    lane = lax.broadcasted_iota(jnp.int32, (dim, dim), 1)
    full = jnp.broadcast_to(row, (dim, dim))
    return jnp.sum(jnp.where(sub == lane, full, 0.0), axis=1, keepdims=True)


def pick_rows(rows, shape):
    sub = lax.broadcasted_iota(jnp.int32, shape, 0)
    out = jnp.zeros(shape, F32)
    for index, value in enumerate(rows):
        out = jnp.where(sub == index, value, out)
    return out


def prepare(block, scale_ref, rhs_d, rhs_c, vis):
    scaled = block[0:32, :] * scale_ref[...]
    hi, mid, lo = split3(scaled)
    for index, value in enumerate((hi, mid, lo, hi, mid, hi)):
        rhs_d[32 * index : 32 * index + 32, :] = value
    n_hi, n_mid, n_lo = split3(jnp.sum(scaled * scaled, 0, keepdims=True))
    ends = (1.0, 1.0, 1.0, n_hi.astype(F32), n_mid.astype(F32), n_lo.astype(F32))
    rhs_d[192:208, :] = pick_rows(ends, (16, CHUNK)).astype(BF16)
    t_hi, t_lo = split2(block[32:64, :])
    for index, value in enumerate((t_hi, t_lo, t_hi, t_lo)):
        rhs_c[32 * index : 32 * index + 32, :] = value
    for side in (0, CHUNK):
        vis[0:32, side : side + CHUNK] = hi
        vis[32:64, side : side + CHUNK] = mid


def products(lhs_d, lhs_c, rhs_d, rhs_c, dist, coup):
    dist[...] = jnp.dot(lhs_d[:, 0:DEPTH], rhs_d[...], preferred_element_type=F32)
    coup[...] = jnp.dot(lhs_c[...], rhs_c[...], preferred_element_type=F32)


def weigh(dist, coup, w, rows=128):
    for start in range(0, dist.shape[0], rows):
        part = pl.ds(start, rows)
        d2 = jnp.maximum(dist[part, :], 1e-30)
        u = d2 * lax.rsqrt(d2)
        weight = (1.0 / LN2 + u) * jnp.exp2(-u) * coup[part, :]
        hi, lo = split2(weight)
        w[part, 0:CHUNK] = hi
        w[part, CHUNK : 2 * CHUNK] = lo


def gather_sums(vis, w, total):
    total[...] += lax.dot_general(
        vis[...], w[...], (((1,), (1,)), ((), ())), preferred_element_type=F32
    )


def own_side(buf, scale_ref, lhs_d, lhs_c, chunks, probe_count):
    sub = lax.broadcasted_iota(jnp.int32, (32, CHUNK), 0)
    for q in range(chunks):
        block = buf[OWN, q]
        scaled = block[0:32, :] * scale_ref[...]
        hi, mid, lo = (-2.0 * v.astype(F32) for v in split3(scaled))
        norm = [v.astype(F32) for v in split3(jnp.sum(scaled * scaled, 0, keepdims=True))]
        ends = pick_rows((*norm, 1.0, 1.0, 1.0), (64, CHUNK))
        stack = jnp.concatenate([hi, hi, hi, mid, mid, lo, ends], 0)
        lhs_d[q * CHUNK : (q + 1) * CHUNK, :] = stack.T.astype(BF16)
        swapped = jnp.concatenate([block[48:64, :], block[32:48, :]], 0)
        half_inv = LN2 / (2.0 * probe_count)
        table = jnp.where(
            sub == probe_count,
            LN2 * swapped,
            jnp.where(sub == 2 * probe_count + 1, 0.0, -half_inv * swapped),
        )
        t_hi, t_lo = (v.astype(F32) for v in split2(table))
        stack = jnp.concatenate([t_hi, t_hi, t_lo, t_lo], 0)
        lhs_c[q * CHUNK : (q + 1) * CHUNK, :] = stack.T.astype(BF16)


def kernel(size, coords, alpha, solves, probes, length, out, *scratch):
    (buf, scale_ref, lhs_d, lhs_c, rhs_d0, rhs_d1, rhs_c0, rhs_c1, v0, v1, v2, v3,
     dist0, dist1, coup0, coup1, w0, w1, total, send_sem, recv_sem) = scratch
    rhs_d, rhs_c, vis = (rhs_d0, rhs_d1), (rhs_c0, rhs_c1), (v0, v1, v2, v3)
    dist, coup, w = (dist0, dist1), (coup0, coup1), (w0, w1)
    dim, points = coords.shape
    probe_count = solves.shape[0]
    chunks = points // CHUNK
    hops = size // 8
    passes = hops * chunks

    group = lax.axis_index("groups")
    me = lax.axis_index("blk")
    core = lax.rem(me, 2)
    above = lax.rem(me + 2, size)
    below = lax.rem(me + size - 2, size)
    partner = me + 1 - 2 * core

    for q in range(chunks):
        lanes = slice(q * CHUNK, (q + 1) * CHUNK)
        buf[OWN, q, 0:32, :] = coords[:, lanes]
        buf[OWN, q, 32:64, :] = jnp.concatenate(
            [solves[:, lanes], alpha[:, lanes], probes[:, lanes], alpha[:, lanes]], 0
        )

    barrier = pltpu.get_barrier_semaphore()
    for other in (above, below, partner):
        pl.semaphore_signal(barrier, inc=1, device_id=(group, other), device_id_type=MESH)
    pl.semaphore_wait(barrier, 3)

    def send(src, dst, q, other):
        return pltpu.make_async_remote_copy(
            src_ref=buf.at[src, q],
            dst_ref=buf.at[dst, q],
            send_sem=send_sem.at[dst, q],
            recv_sem=recv_sem.at[dst, q],
            device_id=(group, other),
            device_id_type=MESH,
        )

    def arrived(slot, q):
        send(slot, slot, q, partner).wait_recv()

    for q in range(chunks):
        send(OWN, UP, q, above).start()
        send(OWN, DOWN, q, below).start()
        send(OWN, PARTNER, q, partner).start()

    give_src = jnp.where(core == 0, DOWN + hops - 1, UP + hops - 1)
    give_dst = jnp.where(core == 0, P_DOWN + hops - 1, P_UP + hops - 1)
    take = jnp.where(core == 0, P_UP + hops - 1, P_DOWN + hops - 1)

    def relay(k):
        hop, q = k // chunks, lax.rem(k, chunks)
        arrived(UP + hop, q)

        @pl.when(hop < hops - 1)
        def _():
            send(UP + hop, UP + hop + 1, q, above).start()

        arrived(DOWN + hop, q)

        @pl.when(hop < hops - 1)
        def _():
            send(DOWN + hop, DOWN + hop + 1, q, below).start()
            send(UP + hop, P_UP + hop, q, partner).start()
            send(DOWN + hop, P_DOWN + hop, q, partner).start()

        @pl.when(hop == hops - 1)
        def _():
            send(give_src, give_dst, q, partner).start()

    def extra(e):
        pair = jnp.maximum(e - chunks, 0)
        k = pair // 2
        lane = jnp.where(lax.rem(pair, 2) == 0, P_UP, P_DOWN)
        tail = e - chunks - 2 * (passes - chunks)
        slot = jnp.where(
            e < chunks,
            PARTNER,
            jnp.where(tail < 0, lane + k // chunks, take),
        )
        q = jnp.where(e < chunks, e, jnp.where(tail < 0, lax.rem(k, chunks), tail))
        return slot, q

    def place(k, position):
        e_slot, e_q = extra(2 * k + (1 if position else 0))
        hop, q = k // chunks, lax.rem(k, chunks)
        if position == 0:
            return e_slot, e_q
        last = k == passes - 1
        order = {1: (e_slot, UP + hop), 2: (UP + hop, DOWN + hop), 3: (DOWN + hop, e_slot)}
        q_order = {1: (e_q, q), 2: (q, q), 3: (q, e_q)}
        return (
            jnp.where(last, order[position][1], order[position][0]),
            jnp.where(last, q_order[position][1], q_order[position][0]),
        )

    def ready(k, position):
        slot, q = place(k, position)
        if position == 0:
            @pl.when(k > 0)
            def _():
                relay(k)

            arrived(slot, q)
        elif position == 1:
            @pl.when(k < passes - 1)
            def _():
                arrived(slot, q)
        elif position == 2:
            @pl.when(k == 0)
            def _():
                relay(k)
        else:
            @pl.when(k == passes - 1)
            def _():
                arrived(slot, q)

    def prep(k, position):
        slot, q = place(k, position)
        prepare(buf[slot, q], scale_ref, rhs_d[position % 2], rhs_c[position % 2], vis[position])

    inverse = 1.0 / column_of(length[...], dim)
    scale_ref[...] = jnp.broadcast_to(inverse * UNIT, (dim, CHUNK))
    own_side(buf, scale_ref, lhs_d, lhs_c, chunks, probe_count)
    total[...] = jnp.zeros_like(total)
    w1[...] = jnp.zeros_like(w1)
    sub = lax.broadcasted_iota(jnp.int32, (16, 2 * CHUNK), 0)
    for v in vis:
        v[64:80, :] = jnp.where(sub == 0, 1.0, 0.0).astype(BF16)
    v3[0:64, :] = jnp.zeros((64, 2 * CHUNK), BF16)

    ready(0, 0)
    prep(0, 0)
    products(lhs_d, lhs_c, rhs_d0, rhs_c0, dist0, coup0)
    ready(0, 1)
    prep(0, 1)

    @pl.loop(0, passes)
    def _(k):
        for position in range(4):
            here, there = position % 2, (position + 1) % 2
            ahead = (position + 2) % 4
            if position < 2:
                k_ahead = k
                ready(k, ahead)
            else:
                k_ahead = jnp.minimum(k + 1, passes - 1)

                @pl.when(k < passes - 1)
                def _():
                    ready(k + 1, ahead)

            gather_sums(vis[(position + 3) % 4], w[there], total)
            products(lhs_d, lhs_c, rhs_d[there], rhs_c[there], dist[there], coup[there])
            weigh(dist[here], coup[here], w[here])
            prep(k_ahead, ahead)

    gather_sums(v3, w1, total)

    for q in range(chunks):
        lanes = slice(q * CHUNK, (q + 1) * CHUNK)
        scaled = buf[OWN, q, 0:32, :] * scale_ref[...]
        summed = scaled * total[64:65, lanes] - (total[0:32, lanes] + total[32:64, lanes])
        out[:, lanes] = scale_ref[...] * (-5.0 / (3.0 * UNIT * UNIT)) * summed

    for q in range(chunks):
        send(OWN, PARTNER, q, partner).wait_send()
        for hop in range(hops):
            send(OWN, UP + hop, q, above).wait_send()
            send(OWN, DOWN + hop, q, below).wait_send()
            if hop < hops - 1:
                send(OWN, P_UP + hop, q, partner).wait_send()
                send(OWN, P_DOWN + hop, q, partner).wait_send()
        send(give_src, give_dst, q, partner).wait_send()


def scratch_shapes(dim, points):
    chunks = points // CHUNK
    return [
        pltpu.VMEM((SLOTS, chunks, 64, CHUNK), F32),
        pltpu.VMEM((dim, CHUNK), F32),
        pltpu.VMEM((points, 256), BF16),
        pltpu.VMEM((points, 128), BF16),
        *[pltpu.VMEM((DEPTH, CHUNK), BF16)] * 2,
        *[pltpu.VMEM((128, CHUNK), BF16)] * 2,
        *[pltpu.VMEM((80, 2 * CHUNK), BF16)] * 4,
        *[pltpu.VMEM((points, CHUNK), F32)] * 4,
        *[pltpu.VMEM((points, 2 * CHUNK), BF16)] * 2,
        pltpu.VMEM((80, points), F32),
        pltpu.SemaphoreType.DMA((SLOTS, chunks)),
        pltpu.SemaphoreType.DMA((SLOTS, chunks)),
    ]


def on_device(coords, alpha, probe_solves, probes, lengthscale):
    dim, points = coords.shape
    vmem_spec = pl.BlockSpec(memory_space=pltpu.VMEM)
    return pl.pallas_call(
        functools.partial(kernel, lax.axis_size("blk")),
        out_shape=jax.ShapeDtypeStruct((dim, points), F32),
        in_specs=[vmem_spec] * 5,
        out_specs=vmem_spec,
        scratch_shapes=scratch_shapes(dim, points),
        compiler_params=pltpu.CompilerParams(collective_id=0, has_side_effects=True),
    )(coords, alpha[None], probe_solves, probes, lengthscale[None])


def solution(mesh):
    return jax.shard_map(
        on_device,
        mesh=mesh,
        in_specs=(
            P(None, ("groups", "blk")),
            P(("groups", "blk")),
            P(None, ("groups", "blk")),
            P(None, ("groups", "blk")),
            P(),
        ),
        out_specs=P(None, ("groups", "blk")),
        check_vma=False,
    )
```

```python
import functools
import math

import jax
import jax.numpy as jnp
from jax import lax
from jax.experimental import pallas as pl
from jax.experimental.pallas import tpu as pltpu
from jax.sharding import PartitionSpec as P

F32 = jnp.float32
BF16 = jnp.bfloat16
MESH = pl.DeviceIdType.MESH

UNIT = math.sqrt(5.0) * math.log2(math.e)
LN2 = math.log(2.0)

CHUNK = 256
DEPTH = 208
OWN, PARTNER, UP, DOWN, P_UP, P_DOWN, SLOTS = 0, 1, 2, 6, 10, 14, 18


def split3(x):
    hi = x.astype(BF16)
    rest = x - hi.astype(F32)
    mid = rest.astype(BF16)
    lo = (rest - mid.astype(F32)).astype(BF16)
    return hi, mid, lo


def split2(x):
    hi = x.astype(BF16)
    return hi, (x - hi.astype(F32)).astype(BF16)


def column_of(row, dim):
    sub = lax.broadcasted_iota(jnp.int32, (dim, dim), 0)
    lane = lax.broadcasted_iota(jnp.int32, (dim, dim), 1)
    full = jnp.broadcast_to(row, (dim, dim))
    return jnp.sum(jnp.where(sub == lane, full, 0.0), axis=1, keepdims=True)


def pick_rows(rows, shape):
    sub = lax.broadcasted_iota(jnp.int32, shape, 0)
    out = jnp.zeros(shape, F32)
    for index, value in enumerate(rows):
        out = jnp.where(sub == index, value, out)
    return out


def prepare(block, scale_ref, lhs_d, lhs_c, vis):
    scaled = block[0:32, :] * scale_ref[...]
    hi, mid, lo = split3(scaled)
    norm = [v.astype(F32) for v in split3(jnp.sum(scaled * scaled, 0, keepdims=True))]
    ends = pick_rows((1.0, 1.0, 1.0, *norm), (64, CHUNK)).astype(BF16)
    lhs_d[...] = jnp.concatenate([hi, mid, lo, hi, mid, hi, ends], 0).T
    t_hi, t_lo = split2(block[32:64, :])
    lhs_c[...] = jnp.concatenate([t_hi, t_lo, t_hi, t_lo], 0).T
    for side in (0, CHUNK):
        vis[0:32, side : side + CHUNK] = hi
        vis[32:64, side : side + CHUNK] = mid


def products(lhs_d, lhs_c, rhs_d, rhs_c, dist, coup, lanes):
    dist[:, lanes] = jnp.dot(lhs_d[:, 0:DEPTH], rhs_d[:, lanes], preferred_element_type=F32)
    coup[:, lanes] = jnp.dot(lhs_c[...], rhs_c[:, lanes], preferred_element_type=F32)


def weigh(dist, coup, w, rows, lanes):
    d2 = jnp.maximum(dist[rows, lanes], 1e-30)
    u = d2 * lax.rsqrt(d2)
    weight = (1.0 / LN2 + u) * jnp.exp2(-u) * coup[rows, lanes]
    hi, lo = split2(weight)
    w[rows, lanes] = hi
    w[rows.start + CHUNK : rows.stop + CHUNK, lanes] = lo


def gather_sums(vis, w, total, lanes):
    total[:, lanes] += jnp.dot(vis[...], w[:, lanes], preferred_element_type=F32)


def region(vis, w_old, total, lhs_d, lhs_c, rhs_d, rhs_c, dist, coup, dist_old, coup_old, w, prep):
    def dots(r, n=256):
        products(lhs_d, lhs_c, rhs_d, rhs_c, dist, coup, slice(r, r + n))
    def gat(r, n=256):
        gather_sums(vis, w_old, total, slice(r, r + n))
    def wei(l, n=256, r=0, m=256, step=32):
        for t in range(r, r + m, step):
            weigh(dist_old, coup_old, w, slice(t, t + step), slice(l, l + n))
    for t in range(0, 768, 256):
        dots(t)
        gat(t)
        wei(t)
    prep()

def own_side(buf, scale_ref, rhs_d, rhs_c, chunks, probe_count):
    sub = lax.broadcasted_iota(jnp.int32, (32, CHUNK), 0)
    for q in range(chunks):
        lanes = slice(q * CHUNK, (q + 1) * CHUNK)
        block = buf[OWN, q]
        scaled = block[0:32, :] * scale_ref[...]
        hi, mid, lo = ((-2.0 * v.astype(F32)).astype(BF16) for v in split3(scaled))
        norm = [v.astype(F32) for v in split3(jnp.sum(scaled * scaled, 0, keepdims=True))]
        ends = pick_rows((*norm, 1.0, 1.0, 1.0), (16, CHUNK)).astype(BF16)
        rhs_d[:, lanes] = jnp.concatenate([hi, hi, hi, mid, mid, lo, ends], 0)
        swapped = jnp.concatenate([block[48:64, :], block[32:48, :]], 0)
        half_inv = LN2 / (2.0 * probe_count)
        table = jnp.where(
            sub == probe_count,
            LN2 * swapped,
            jnp.where(sub == 2 * probe_count + 1, 0.0, -half_inv * swapped),
        )
        t_hi, t_lo = split2(table)
        rhs_c[:, lanes] = jnp.concatenate([t_hi, t_hi, t_lo, t_lo], 0)


def kernel(size, coords, alpha, solves, probes, length, out, *scratch):
    (buf, scale_ref, rhs_d, rhs_c, lhs_d0, lhs_d1, lhs_c0, lhs_c1, v0, v1, v2, v3,
     dist0, dist1, coup0, coup1, w0, w1, total, send_sem, recv_sem) = scratch
    lhs_d, lhs_c, vis = (lhs_d0, lhs_d1), (lhs_c0, lhs_c1), (v0, v1, v2, v3)
    dist, coup, w = (dist0, dist1), (coup0, coup1), (w0, w1)
    dim, points = coords.shape
    probe_count = solves.shape[0]
    chunks = points // CHUNK
    hops = size // 8
    passes = hops * chunks

    group = lax.axis_index("groups")
    me = lax.axis_index("blk")
    core = lax.rem(me, 2)
    above = lax.rem(me + 2, size)
    below = lax.rem(me + size - 2, size)
    partner = me + 1 - 2 * core

    for q in range(chunks):
        lanes = slice(q * CHUNK, (q + 1) * CHUNK)
        row = alpha[lanes].reshape(1, CHUNK)
        buf[OWN, q, 0:32, :] = coords[:, lanes]
        buf[OWN, q, 32:64, :] = jnp.concatenate(
            [solves[:, lanes], row, probes[:, lanes], row], 0
        )

    barrier = pltpu.get_barrier_semaphore()
    for other in (above, below, partner):
        pl.semaphore_signal(barrier, inc=1, device_id=(group, other), device_id_type=MESH)
    pl.semaphore_wait(barrier, 3)

    def send(src, dst, q, other):
        return pltpu.make_async_remote_copy(
            src_ref=buf.at[src, q],
            dst_ref=buf.at[dst, q],
            send_sem=send_sem.at[dst, q],
            recv_sem=recv_sem.at[dst, q],
            device_id=(group, other),
            device_id_type=MESH,
        )

    def arrived(slot, q):
        send(slot, slot, q, partner).wait_recv()

    for q in range(chunks):
        send(OWN, UP, q, above).start()
        send(OWN, DOWN, q, below).start()
        send(OWN, PARTNER, q, partner).start()

    give_src = jnp.where(core == 0, DOWN + hops - 1, UP + hops - 1)
    give_dst = jnp.where(core == 0, P_DOWN + hops - 1, P_UP + hops - 1)
    take = jnp.where(core == 0, P_UP + hops - 1, P_DOWN + hops - 1)

    def relay(k):
        hop, q = k // chunks, lax.rem(k, chunks)
        arrived(UP + hop, q)

        @pl.when(hop < hops - 1)
        def _():
            send(UP + hop, UP + hop + 1, q, above).start()

        arrived(DOWN + hop, q)

        @pl.when(hop < hops - 1)
        def _():
            send(DOWN + hop, DOWN + hop + 1, q, below).start()
            send(UP + hop, P_UP + hop, q, partner).start()
            send(DOWN + hop, P_DOWN + hop, q, partner).start()

        @pl.when(hop == hops - 1)
        def _():
            send(give_src, give_dst, q, partner).start()

    def extra(e):
        pair = jnp.maximum(e - chunks, 0)
        k = pair // 2
        lane = jnp.where(lax.rem(pair, 2) == 0, P_UP, P_DOWN)
        tail = e - chunks - 2 * (passes - chunks)
        slot = jnp.where(
            e < chunks,
            PARTNER,
            jnp.where(tail < 0, lane + k // chunks, take),
        )
        q = jnp.where(e < chunks, e, jnp.where(tail < 0, lax.rem(k, chunks), tail))
        return slot, q

    def place(k, position):
        e_slot, e_q = extra(2 * k + (1 if position else 0))
        hop, q = k // chunks, lax.rem(k, chunks)
        if position == 0:
            return e_slot, e_q
        last = k == passes - 1
        order = {1: (e_slot, UP + hop), 2: (UP + hop, DOWN + hop), 3: (DOWN + hop, e_slot)}
        q_order = {1: (e_q, q), 2: (q, q), 3: (q, e_q)}
        return (
            jnp.where(last, order[position][1], order[position][0]),
            jnp.where(last, q_order[position][1], q_order[position][0]),
        )

    def ready(k, position):
        slot, q = place(k, position)
        if position == 0:
            @pl.when(k > 0)
            def _():
                relay(k)

            arrived(slot, q)
        elif position == 1:
            @pl.when(k < passes - 1)
            def _():
                arrived(slot, q)
        elif position == 2:
            @pl.when(k == 0)
            def _():
                relay(k)
        else:
            @pl.when(k == passes - 1)
            def _():
                arrived(slot, q)

    def prep(k, position):
        slot, q = place(k, position)
        prepare(buf[slot, q], scale_ref, lhs_d[position % 2], lhs_c[position % 2], vis[position])

    inverse = 1.0 / column_of(length[...], dim)
    scale_ref[...] = jnp.broadcast_to(inverse * UNIT, (dim, CHUNK))
    own_side(buf, scale_ref, rhs_d, rhs_c, chunks, probe_count)
    total[...] = jnp.zeros_like(total)
    w1[...] = jnp.zeros_like(w1)
    sub = lax.broadcasted_iota(jnp.int32, (16, 2 * CHUNK), 0)
    for v in vis:
        v[64:80, :] = jnp.where(sub == 0, 1.0, 0.0).astype(BF16)
    v3[0:64, :] = jnp.zeros((64, 2 * CHUNK), BF16)

    ready(0, 0)
    prep(0, 0)
    products(lhs_d0, lhs_c0, rhs_d, rhs_c, dist0, coup0, slice(0, points))
    ready(0, 1)
    prep(0, 1)

    @pl.loop(0, passes)
    def _(k):
        for position in range(4):
            here, there = position % 2, (position + 1) % 2
            ahead = (position + 2) % 4
            if position == 0:
                ready(k, 2)
                ready(k, 3)
            elif position == 2:
                @pl.when(k < passes - 1)
                def _():
                    ready(k + 1, 0)
                    ready(k + 1, 1)
            k_ahead = k if position < 2 else jnp.minimum(k + 1, passes - 1)
            region(vis[(position + 3) % 4], w[there], total, lhs_d[there], lhs_c[there], rhs_d, rhs_c,
                   dist[there], coup[there], dist[here], coup[here], w[here],
                   lambda: prep(k_ahead, ahead))

    gather_sums(v3, w1, total, slice(0, points))

    for q in range(chunks):
        lanes = slice(q * CHUNK, (q + 1) * CHUNK)
        scaled = buf[OWN, q, 0:32, :] * scale_ref[...]
        summed = scaled * total[64:65, lanes] - (total[0:32, lanes] + total[32:64, lanes])
        out[:, lanes] = scale_ref[...] * (-5.0 / (3.0 * UNIT * UNIT)) * summed

    for q in range(chunks):
        send(OWN, PARTNER, q, partner).wait_send()
        for hop in range(hops):
            send(OWN, UP + hop, q, above).wait_send()
            send(OWN, DOWN + hop, q, below).wait_send()
            if hop < hops - 1:
                send(OWN, P_UP + hop, q, partner).wait_send()
                send(OWN, P_DOWN + hop, q, partner).wait_send()
        send(give_src, give_dst, q, partner).wait_send()


def scratch_shapes(dim, points):
    chunks = points // CHUNK
    return [
        pltpu.VMEM((SLOTS, chunks, 64, CHUNK), F32),
        pltpu.VMEM((dim, CHUNK), F32),
        pltpu.VMEM((DEPTH, points), BF16),
        pltpu.VMEM((128, points), BF16),
        *[pltpu.VMEM((CHUNK, 256), BF16)] * 2,
        *[pltpu.VMEM((CHUNK, 128), BF16)] * 2,
        *[pltpu.VMEM((80, 2 * CHUNK), BF16)] * 4,
        *[pltpu.VMEM((CHUNK, points), F32)] * 4,
        *[pltpu.VMEM((2 * CHUNK, points), BF16)] * 2,
        pltpu.VMEM((80, points), F32),
        pltpu.SemaphoreType.DMA((SLOTS, chunks)),
        pltpu.SemaphoreType.DMA((SLOTS, chunks)),
    ]


def on_device(coords, alpha, probe_solves, probes, lengthscale):
    dim, points = coords.shape
    vmem_spec = pl.BlockSpec(memory_space=pltpu.VMEM)
    return pl.pallas_call(
        functools.partial(kernel, lax.axis_size("blk")),
        out_shape=jax.ShapeDtypeStruct((dim, points), F32),
        in_specs=[vmem_spec] * 5,
        out_specs=vmem_spec,
        scratch_shapes=scratch_shapes(dim, points),
        compiler_params=pltpu.CompilerParams(collective_id=0, has_side_effects=True),
    )(coords, alpha, probe_solves, probes, lengthscale[None])


def solution(mesh):
    return jax.shard_map(
        on_device,
        mesh=mesh,
        in_specs=(
            P(None, ("groups", "blk")),
            P(("groups", "blk")),
            P(None, ("groups", "blk")),
            P(None, ("groups", "blk")),
            P(),
        ),
        out_specs=P(None, ("groups", "blk")),
        check_vma=False,
    )
```

```python
import functools
import math

import jax
import jax.numpy as jnp
from jax import lax
from jax.experimental import pallas as pl
from jax.experimental.pallas import tpu as pltpu
from jax.sharding import PartitionSpec as P

F32 = jnp.float32
BF16 = jnp.bfloat16
MESH = pl.DeviceIdType.MESH

UNIT = math.sqrt(5.0) * math.log2(math.e)
LN2 = math.log(2.0)

CHUNK = 256
DEPTH = 208
OWN, PARTNER, UP, DOWN, P_UP, P_DOWN, SLOTS = 0, 1, 2, 6, 10, 14, 18


def split3(x):
    hi = x.astype(BF16)
    rest = x - hi.astype(F32)
    mid = rest.astype(BF16)
    lo = (rest - mid.astype(F32)).astype(BF16)
    return hi, mid, lo


def split2(x):
    hi = x.astype(BF16)
    return hi, (x - hi.astype(F32)).astype(BF16)


def column_of(row, dim):
    sub = lax.broadcasted_iota(jnp.int32, (dim, dim), 0)
    lane = lax.broadcasted_iota(jnp.int32, (dim, dim), 1)
    full = jnp.broadcast_to(row, (dim, dim))
    return jnp.sum(jnp.where(sub == lane, full, 0.0), axis=1, keepdims=True)


def pick_rows(rows, shape):
    sub = lax.broadcasted_iota(jnp.int32, shape, 0)
    out = jnp.zeros(shape, F32)
    for index, value in enumerate(rows):
        out = jnp.where(sub == index, value, out)
    return out


def prepare(block, scale_ref, lhs_d, lhs_c, vis):
    scaled = block[0:32, :] * scale_ref[...]
    hi, mid, lo = split3(scaled)
    norm = [v.astype(F32) for v in split3(jnp.sum(scaled * scaled, 0, keepdims=True))]
    ends = pick_rows((1.0, 1.0, 1.0, *norm), (8, CHUNK))
    ends = jnp.concatenate([ends, jnp.zeros((8, CHUNK), F32)], 0).astype(BF16)
    rest = jnp.zeros((256 - DEPTH, CHUNK), BF16)
    lhs_d[...] = jnp.concatenate([hi, mid, lo, hi, mid, hi, ends, rest], 0).T
    t_hi, t_lo = split2(block[32:64, :])
    lhs_c[...] = jnp.concatenate([t_hi, t_lo, t_hi, t_lo], 0).T
    for side in (0, CHUNK):
        vis[0:32, side : side + CHUNK] = hi
        vis[32:64, side : side + CHUNK] = mid


def products(lhs_d, lhs_c, rhs_d, rhs_c, dist, coup, lanes):
    d2 = jnp.dot(lhs_d[:, 0:DEPTH], rhs_d[:, lanes], preferred_element_type=F32)
    dist[:, lanes] = jnp.maximum(d2, 1e-30)
    coup[:, lanes] = jnp.dot(lhs_c[...], rhs_c[:, lanes], preferred_element_type=F32)


def weigh(dist, coup, w, rows, lanes):
    d2 = dist[rows, lanes]
    u = d2 * lax.rsqrt(d2)
    weight = (1.0 / LN2 + u) * jnp.exp2(-u) * coup[rows, lanes]
    hi, lo = split2(weight)
    w[rows, lanes] = hi
    w[rows.start + CHUNK : rows.stop + CHUNK, lanes] = lo


def gather_sums(vis, w, total, lanes):
    total[:, lanes] += jnp.dot(vis[...], w[:, lanes], preferred_element_type=F32)


def region(vis, w_old, total, lhs_d, lhs_c, rhs_d, rhs_c, dist, coup, dist_old, coup_old, w, prep, products_ahead):
    def dots(r, n=256):
        products(lhs_d, lhs_c, rhs_d, rhs_c, dist, coup, slice(r, r + n))
    def gat(r, n=256):
        gather_sums(vis, w_old, total, slice(r, r + n))
    def wei(l, n=256, r=0, m=256, step=32):
        for t in range(r, r + m, step):
            weigh(dist_old, coup_old, w, slice(t, t + step), slice(l, l + n))
    for t in range(0, w.shape[1], CHUNK):
        if products_ahead:
            dots(t)
        gat(t)
        wei(t)
    if prep is not None:
        prep()


def own_side(buf, scale_ref, rhs_d, rhs_c, chunks, probe_count):
    sub = lax.broadcasted_iota(jnp.int32, (32, CHUNK), 0)
    for q in range(chunks):
        lanes = slice(q * CHUNK, (q + 1) * CHUNK)
        block = buf[OWN, q]
        scaled = block[0:32, :] * scale_ref[...]
        hi, mid, lo = ((-2.0 * v.astype(F32)).astype(BF16) for v in split3(scaled))
        norm = [v.astype(F32) for v in split3(jnp.sum(scaled * scaled, 0, keepdims=True))]
        ends = pick_rows((*norm, 1.0, 1.0, 1.0), (16, CHUNK)).astype(BF16)
        rhs_d[:, lanes] = jnp.concatenate([hi, hi, hi, mid, mid, lo, ends], 0)
        swapped = jnp.concatenate([block[48:64, :], block[32:48, :]], 0)
        half_inv = LN2 / (2.0 * probe_count)
        table = jnp.where(
            sub == probe_count,
            LN2 * swapped,
            jnp.where(sub == 2 * probe_count + 1, 0.0, -half_inv * swapped),
        )
        t_hi, t_lo = split2(table)
        rhs_c[:, lanes] = jnp.concatenate([t_hi, t_hi, t_lo, t_lo], 0)


def kernel(size, coords_in, alpha_in, solves_in, probes_in, length_in, out, *scratch):
    (buf, scale_ref, rhs_d, rhs_c, lhs_d0, lhs_d1, lhs_c0, lhs_c1, v0, v1, v2, v3,
     dist0, dist1, coup0, coup1, w0, w1, total, coords, alpha, solves, probes, length,
     in_sem, send_sem, recv_sem) = scratch
    lhs_d, lhs_c, vis = (lhs_d0, lhs_d1), (lhs_c0, lhs_c1), (v0, v1, v2, v3)
    dist, coup, w = (dist0, dist1), (coup0, coup1), (w0, w1)
    dim, points = coords.shape
    probe_count = solves.shape[0]
    chunks = points // CHUNK
    hops = size // 8
    passes = hops * chunks

    group = lax.axis_index("groups")
    me = lax.axis_index("blk")
    core = lax.rem(me, 2)
    above = lax.rem(me + 2, size)
    below = lax.rem(me + size - 2, size)
    partner = me + 1 - 2 * core

    barrier = pltpu.get_barrier_semaphore()
    for other in (above, below, partner):
        pl.semaphore_signal(barrier, inc=1, device_id=(group, other), device_id_type=MESH)

    loads = [
        pltpu.make_async_copy(src, dst, in_sem.at[index])
        for index, (src, dst) in enumerate(
            ((coords_in, coords), (alpha_in, alpha), (solves_in, solves), (probes_in, probes),
             (length_in, length))
        )
    ]
    for load in loads:
        load.start()
    for load in loads:
        load.wait()

    for q in range(chunks):
        lanes = slice(q * CHUNK, (q + 1) * CHUNK)
        row = alpha[lanes].reshape(1, CHUNK)
        buf[OWN, q, 0:32, :] = coords[:, lanes]
        buf[OWN, q, 32:64, :] = jnp.concatenate(
            [solves[:, lanes], row, probes[:, lanes], row], 0
        )

    pl.semaphore_wait(barrier, 3)

    def send(src, dst, q, other):
        return pltpu.make_async_remote_copy(
            src_ref=buf.at[src, q],
            dst_ref=buf.at[dst, q],
            send_sem=send_sem.at[dst, q],
            recv_sem=recv_sem.at[dst, q],
            device_id=(group, other),
            device_id_type=MESH,
        )

    def arrived(slot, q):
        send(slot, slot, q, partner).wait_recv()

    for q in range(chunks):
        send(OWN, UP, q, above).start()
        send(OWN, DOWN, q, below).start()
        send(OWN, PARTNER, q, partner).start()

    give_src = jnp.where(core == 0, DOWN + hops - 1, UP + hops - 1)
    give_dst = jnp.where(core == 0, P_DOWN + hops - 1, P_UP + hops - 1)
    take = jnp.where(core == 0, P_UP + hops - 1, P_DOWN + hops - 1)

    def relay(k, last_hop):
        hop, q = k // chunks, lax.rem(k, chunks)
        arrived(UP + hop, q)
        if not last_hop:
            send(UP + hop, UP + hop + 1, q, above).start()
        arrived(DOWN + hop, q)
        if last_hop:
            send(give_src, give_dst, q, partner).start()
        else:
            send(DOWN + hop, DOWN + hop + 1, q, below).start()
            send(UP + hop, P_UP + hop, q, partner).start()
            send(DOWN + hop, P_DOWN + hop, q, partner).start()

    def prep(slot, q, position):
        prepare(buf[slot, q], scale_ref, lhs_d[position % 2], lhs_c[position % 2], vis[position])

    def step(position, slot=None, q=None, more=True):
        here, there = position % 2, (position + 1) % 2
        ahead = None if slot is None else lambda: prep(slot, q, (position + 2) % 4)
        region(vis[(position + 3) % 4], w[there], total, lhs_d[there], lhs_c[there], rhs_d, rhs_c,
               dist[there], coup[there], dist[here], coup[here], w[here], ahead, more)

    def up(k):
        return UP + k // chunks, lax.rem(k, chunks)

    def down(k):
        return DOWN + k // chunks, lax.rem(k, chunks)

    def side(k):
        return (P_UP + k // chunks, lax.rem(k, chunks)), (P_DOWN + k // chunks, lax.rem(k, chunks))

    inverse = 1.0 / column_of(length[...], dim)
    scale_ref[...] = jnp.broadcast_to(inverse * UNIT, (dim, CHUNK))
    own_side(buf, scale_ref, rhs_d, rhs_c, chunks, probe_count)
    total[...] = jnp.zeros_like(total)
    w1[...] = jnp.zeros_like(w1)
    sub = lax.broadcasted_iota(jnp.int32, (16, 2 * CHUNK), 0)
    for v in vis:
        v[64:80, :] = jnp.where(sub == 0, 1.0, 0.0).astype(BF16)
    v3[0:64, :] = jnp.zeros((64, 2 * CHUNK), BF16)

    for q in range(chunks):
        arrived(PARTNER, q)
    prep(PARTNER, 0, 0)
    products(lhs_d0, lhs_c0, rhs_d, rhs_c, dist0, coup0, slice(0, points))
    prep(PARTNER, 1, 1)
    step(0, PARTNER, 2)
    relay(0, False)
    step(1, UP, 0)
    step(2, DOWN, 0)
    relay(1, False)
    step(3, UP, 1)
    step(0, DOWN, 1)

    def turn(k, last_hop):
        left, right = side(k - 1)
        arrived(*left)
        arrived(*right)
        step(1, *left)
        step(2, *right)
        relay(k + 1, last_hop)
        step(3, *up(k + 1))
        step(0, *down(k + 1))

    @pl.loop(1, passes - chunks - 1)
    def _(k):
        turn(k, False)

    @pl.loop(passes - chunks - 1, passes - chunks + 1)
    def _(k):
        turn(k, True)

    arrived(take, 0)
    arrived(take, 1)
    step(1, take, 0)
    step(2, take, 1)
    relay(passes - 1, True)
    step(3, *up(passes - 1))
    step(0, *down(passes - 1))
    arrived(take, 2)
    step(1, take, 2)
    step(2)
    step(3, more=False)
    gather_sums(v3, w1, total, slice(0, points))

    for q in range(chunks):
        lanes = slice(q * CHUNK, (q + 1) * CHUNK)
        scaled = buf[OWN, q, 0:32, :] * scale_ref[...]
        summed = scaled * total[64:65, lanes] - (total[0:32, lanes] + total[32:64, lanes])
        out[:, lanes] = scale_ref[...] * (-5.0 / (3.0 * UNIT * UNIT)) * summed

    for q in range(chunks):
        send(OWN, PARTNER, q, partner).wait_send()
        for hop in range(hops):
            send(OWN, UP + hop, q, above).wait_send()
            send(OWN, DOWN + hop, q, below).wait_send()
            if hop < hops - 1:
                send(OWN, P_UP + hop, q, partner).wait_send()
                send(OWN, P_DOWN + hop, q, partner).wait_send()
        send(give_src, give_dst, q, partner).wait_send()


def scratch_shapes(dim, points, probe_count):
    chunks = points // CHUNK
    return [
        pltpu.VMEM((SLOTS, chunks, 64, CHUNK), F32),
        pltpu.VMEM((dim, CHUNK), F32),
        pltpu.VMEM((DEPTH, points), BF16),
        pltpu.VMEM((128, points), BF16),
        *[pltpu.VMEM((CHUNK, 256), BF16)] * 2,
        *[pltpu.VMEM((CHUNK, 128), BF16)] * 2,
        *[pltpu.VMEM((80, 2 * CHUNK), BF16)] * 4,
        *[pltpu.VMEM((CHUNK, points), F32)] * 4,
        *[pltpu.VMEM((2 * CHUNK, points), BF16)] * 2,
        pltpu.VMEM((80, points), F32),
        pltpu.VMEM((dim, points), F32),
        pltpu.VMEM((points,), F32),
        pltpu.VMEM((probe_count, points), F32),
        pltpu.VMEM((probe_count, points), F32),
        pltpu.VMEM((1, dim), F32),
        pltpu.SemaphoreType.DMA((5,)),
        pltpu.SemaphoreType.DMA((SLOTS, chunks)),
        pltpu.SemaphoreType.DMA((SLOTS, chunks)),
    ]


def on_device(coords, alpha, probe_solves, probes, lengthscale):
    dim, points = coords.shape
    any_spec = pl.BlockSpec(memory_space=pl.ANY)
    vmem_spec = pl.BlockSpec(memory_space=pltpu.VMEM)
    return pl.pallas_call(
        functools.partial(kernel, lax.axis_size("blk")),
        out_shape=jax.ShapeDtypeStruct((dim, points), F32),
        in_specs=[any_spec] * 5,
        out_specs=vmem_spec,
        scratch_shapes=scratch_shapes(dim, points, probe_solves.shape[0]),
        compiler_params=pltpu.CompilerParams(collective_id=0, has_side_effects=True),
    )(coords, alpha, probe_solves, probes, lengthscale[None])


def solution(mesh):
    return jax.shard_map(
        on_device,
        mesh=mesh,
        in_specs=(
            P(None, ("groups", "blk")),
            P(("groups", "blk")),
            P(None, ("groups", "blk")),
            P(None, ("groups", "blk")),
            P(),
        ),
        out_specs=P(None, ("groups", "blk")),
        check_vma=False,
    )
```

```python
import functools
import math

import jax
import jax.numpy as jnp
from jax import lax
from jax.experimental import pallas as pl
from jax.experimental.pallas import tpu as pltpu
from jax.sharding import PartitionSpec as P

F32 = jnp.float32
BF16 = jnp.bfloat16
MESH = pl.DeviceIdType.MESH

UNIT = math.sqrt(5.0) * math.log2(math.e)
LN2 = math.log(2.0)

CHUNK = 256
DEPTH = 208
OWN, PARTNER, UP, DOWN, P_UP, P_DOWN, SLOTS = 0, 1, 2, 6, 10, 14, 18


def split3(x):
    hi = x.astype(BF16)
    rest = x - hi.astype(F32)
    mid = rest.astype(BF16)
    lo = (rest - mid.astype(F32)).astype(BF16)
    return hi, mid, lo


def split2(x):
    hi = x.astype(BF16)
    return hi, (x - hi.astype(F32)).astype(BF16)


def column_of(row, dim):
    sub = lax.broadcasted_iota(jnp.int32, (dim, dim), 0)
    lane = lax.broadcasted_iota(jnp.int32, (dim, dim), 1)
    full = jnp.broadcast_to(row, (dim, dim))
    return jnp.sum(jnp.where(sub == lane, full, 0.0), axis=1, keepdims=True)


def pick_rows(rows, shape):
    sub = lax.broadcasted_iota(jnp.int32, shape, 0)
    out = jnp.zeros(shape, F32)
    for index, value in enumerate(rows):
        out = jnp.where(sub == index, value, out)
    return out


def prepare(block, scale_ref, lhs_d, lhs_c, vis):
    scaled = block[0:32, :] * scale_ref[...]
    hi, mid, lo = split3(scaled)
    norm = [v.astype(F32) for v in split3(jnp.sum(scaled * scaled, 0, keepdims=True))]
    ends = pick_rows((1.0, 1.0, 1.0, *norm), (8, CHUNK))
    ends = jnp.concatenate([ends, jnp.zeros((8, CHUNK), F32)], 0).astype(BF16)
    rest = jnp.zeros((256 - DEPTH, CHUNK), BF16)
    lhs_d[...] = jnp.concatenate([hi, mid, lo, hi, mid, hi, ends, rest], 0).T
    t_hi, t_lo = split2(block[32:64, :])
    lhs_c[...] = jnp.concatenate([t_hi, t_lo, t_hi, t_lo], 0).T
    for side in (0, CHUNK):
        vis[0:32, side : side + CHUNK] = hi
        vis[32:64, side : side + CHUNK] = mid


def direct(lhs_d, lhs_c, rhs_d, rhs_c, w, lanes, floor_ref):
    floor = jnp.concatenate([jnp.concatenate([floor_ref[...]] * (CHUNK // 128), 1)] * 4, 0)
    dist = jnp.dot(lhs_d[:, 0:DEPTH], rhs_d[:, lanes], preferred_element_type=F32)
    coup = jnp.dot(lhs_c[...], rhs_c[:, lanes], preferred_element_type=F32)
    for start in range(0, CHUNK, 32):
        rows = slice(start, start + 32)
        d2 = jnp.maximum(dist[rows], floor)
        u = d2 * lax.rsqrt(d2)
        weight = (1.0 / LN2 + u) * jnp.exp2(-u) * coup[rows]
        w[rows, lanes] = weight.astype(BF16)
        lo = weight - w[rows, lanes].astype(F32)
        w[start + CHUNK : start + 32 + CHUNK, lanes] = lo.astype(BF16)


def gather_sums(vis, w, total, lanes):
    total[:, lanes] += jnp.dot(vis[...], w[:, lanes], preferred_element_type=F32)


def region(lhs_d, lhs_c, rhs_d, rhs_c, vis, vis_old, w, w_old, total, floor_ref, prep):
    if prep is not None:
        prep()
    for t in range(0, w.shape[1], CHUNK):
        lanes = slice(t, t + CHUNK)
        direct(lhs_d, lhs_c, rhs_d, rhs_c, w, lanes, floor_ref)
        gather_sums(vis_old, w_old, total, lanes)


def own_side(buf, scale_ref, rhs_d, rhs_c, chunks, probe_count):
    sub = lax.broadcasted_iota(jnp.int32, (32, CHUNK), 0)
    for q in range(chunks):
        lanes = slice(q * CHUNK, (q + 1) * CHUNK)
        block = buf[OWN, q]
        scaled = block[0:32, :] * scale_ref[...]
        hi, mid, lo = ((-2.0 * v.astype(F32)).astype(BF16) for v in split3(scaled))
        norm = [v.astype(F32) for v in split3(jnp.sum(scaled * scaled, 0, keepdims=True))]
        ends = pick_rows((*norm, 1.0, 1.0, 1.0), (16, CHUNK)).astype(BF16)
        rhs_d[:, lanes] = jnp.concatenate([hi, hi, hi, mid, mid, lo, ends], 0)
        swapped = jnp.concatenate([block[48:64, :], block[32:48, :]], 0)
        half_inv = LN2 / (2.0 * probe_count)
        table = jnp.where(
            sub == probe_count,
            LN2 * swapped,
            jnp.where(sub == 2 * probe_count + 1, 0.0, -half_inv * swapped),
        )
        t_hi, t_lo = split2(table)
        rhs_c[:, lanes] = jnp.concatenate([t_hi, t_hi, t_lo, t_lo], 0)


def kernel(size, coords_in, alpha_in, solves_in, probes_in, length_in, out, *scratch):
    (buf, scale_ref, rhs_d, rhs_c, ld0, ld1, ld2, ld3, lc0, lc1, lc2, lc3, v0, v1, v2, v3,
     w0, w1, total, coords, alpha, solves, probes, length,
     floor_ref, in_sem, send_sem, recv_sem) = scratch
    lhs_d, lhs_c, vis = (ld0, ld1, ld2, ld3), (lc0, lc1, lc2, lc3), (v0, v1, v2, v3)
    w = (w0, w1)
    dim, points = coords.shape
    probe_count = solves.shape[0]
    chunks = points // CHUNK
    hops = size // 8
    passes = hops * chunks

    group = lax.axis_index("groups")
    me = lax.axis_index("blk")
    core = lax.rem(me, 2)
    above = lax.rem(me + 2, size)
    below = lax.rem(me + size - 2, size)
    partner = me + 1 - 2 * core

    barrier = pltpu.get_barrier_semaphore()
    for other in (above, below, partner):
        pl.semaphore_signal(barrier, inc=1, device_id=(group, other), device_id_type=MESH)

    loads = [
        pltpu.make_async_copy(src, dst, in_sem.at[index])
        for index, (src, dst) in enumerate(
            ((coords_in, coords), (alpha_in, alpha), (solves_in, solves), (probes_in, probes),
             (length_in, length))
        )
    ]
    for load in loads:
        load.start()
    for load in loads:
        load.wait()

    for q in range(chunks):
        lanes = slice(q * CHUNK, (q + 1) * CHUNK)
        row = alpha[lanes].reshape(1, CHUNK)
        buf[OWN, q, 0:32, :] = coords[:, lanes]
        buf[OWN, q, 32:64, :] = jnp.concatenate(
            [solves[:, lanes], row, probes[:, lanes], row], 0
        )

    pl.semaphore_wait(barrier, 3)

    def send(src, dst, q, other):
        return pltpu.make_async_remote_copy(
            src_ref=buf.at[src, q],
            dst_ref=buf.at[dst, q],
            send_sem=send_sem.at[dst, q],
            recv_sem=recv_sem.at[dst, q],
            device_id=(group, other),
            device_id_type=MESH,
        )

    def arrived(slot, q):
        send(slot, slot, q, partner).wait_recv()

    for q in range(chunks):
        send(OWN, UP, q, above).start()
        send(OWN, DOWN, q, below).start()
        send(OWN, PARTNER, q, partner).start()

    give_src = jnp.where(core == 0, DOWN + hops - 1, UP + hops - 1)
    give_dst = jnp.where(core == 0, P_DOWN + hops - 1, P_UP + hops - 1)
    take = jnp.where(core == 0, P_UP + hops - 1, P_DOWN + hops - 1)

    def relay(k, last_hop):
        hop, q = k // chunks, lax.rem(k, chunks)
        arrived(UP + hop, q)
        if not last_hop:
            send(UP + hop, UP + hop + 1, q, above).start()
        arrived(DOWN + hop, q)
        if last_hop:
            send(give_src, give_dst, q, partner).start()
        else:
            send(DOWN + hop, DOWN + hop + 1, q, below).start()
            send(UP + hop, P_UP + hop, q, partner).start()
            send(DOWN + hop, P_DOWN + hop, q, partner).start()

    def prep(slot, q, position):
        prepare(buf[slot, q], scale_ref, lhs_d[position], lhs_c[position], vis[position])

    def step(position, slot=None, q=None, more=True):
        here, there = position % 2, (position + 1) % 2
        ahead = None if slot is None else lambda: prep(slot, q, (position + 2) % 4)
        region(lhs_d[position], lhs_c[position], rhs_d, rhs_c, vis[position], vis[(position + 3) % 4],
               w[here], w[there], total, floor_ref, ahead)

    def up(k):
        return UP + k // chunks, lax.rem(k, chunks)

    def down(k):
        return DOWN + k // chunks, lax.rem(k, chunks)

    def side(k):
        return (P_UP + k // chunks, lax.rem(k, chunks)), (P_DOWN + k // chunks, lax.rem(k, chunks))

    inverse = 1.0 / column_of(length[...], dim)
    scale_ref[...] = jnp.broadcast_to(inverse * UNIT, (dim, CHUNK))
    own_side(buf, scale_ref, rhs_d, rhs_c, chunks, probe_count)
    total[...] = jnp.zeros_like(total)
    floor_ref[...] = jnp.full_like(floor_ref, 1e-30)
    w1[...] = jnp.zeros_like(w1)
    sub = lax.broadcasted_iota(jnp.int32, (16, 2 * CHUNK), 0)
    for v in vis:
        v[64:80, :] = jnp.where(sub == 0, 1.0, 0.0).astype(BF16)
    v3[0:64, :] = jnp.zeros((64, 2 * CHUNK), BF16)

    for q in range(chunks):
        arrived(PARTNER, q)
    prep(PARTNER, 0, 0)
    prep(PARTNER, 1, 1)
    step(0, PARTNER, 2)
    relay(0, False)
    step(1, UP, 0)
    step(2, DOWN, 0)
    relay(1, False)
    step(3, UP, 1)
    step(0, DOWN, 1)

    def turn(k, last_hop):
        left, right = side(k - 1)
        arrived(*left)
        arrived(*right)
        step(1, *left)
        step(2, *right)
        relay(k + 1, last_hop)
        step(3, *up(k + 1))
        step(0, *down(k + 1))

    @pl.loop(1, passes - chunks - 1)
    def _(k):
        turn(k, False)

    @pl.loop(passes - chunks - 1, passes - chunks + 1)
    def _(k):
        turn(k, True)

    arrived(take, 0)
    arrived(take, 1)
    step(1, take, 0)
    step(2, take, 1)
    relay(passes - 1, True)
    step(3, *up(passes - 1))
    step(0, *down(passes - 1))
    arrived(take, 2)
    step(1, take, 2)
    step(2)
    step(3, more=False)
    gather_sums(v3, w1, total, slice(0, points))

    for q in range(chunks):
        lanes = slice(q * CHUNK, (q + 1) * CHUNK)
        scaled = buf[OWN, q, 0:32, :] * scale_ref[...]
        summed = scaled * total[64:65, lanes] - (total[0:32, lanes] + total[32:64, lanes])
        out[:, lanes] = scale_ref[...] * (-5.0 / (3.0 * UNIT * UNIT)) * summed

    for q in range(chunks):
        send(OWN, PARTNER, q, partner).wait_send()
        for hop in range(hops):
            send(OWN, UP + hop, q, above).wait_send()
            send(OWN, DOWN + hop, q, below).wait_send()
            if hop < hops - 1:
                send(OWN, P_UP + hop, q, partner).wait_send()
                send(OWN, P_DOWN + hop, q, partner).wait_send()
        send(give_src, give_dst, q, partner).wait_send()


def scratch_shapes(dim, points, probe_count):
    chunks = points // CHUNK
    return [
        pltpu.VMEM((SLOTS, chunks, 64, CHUNK), F32),
        pltpu.VMEM((dim, CHUNK), F32),
        pltpu.VMEM((DEPTH, points), BF16),
        pltpu.VMEM((128, points), BF16),
        *[pltpu.VMEM((CHUNK, 256), BF16)] * 4,
        *[pltpu.VMEM((CHUNK, 128), BF16)] * 4,
        *[pltpu.VMEM((80, 2 * CHUNK), BF16)] * 4,
        *[pltpu.VMEM((2 * CHUNK, points), BF16)] * 2,
        pltpu.VMEM((80, points), F32),
        pltpu.VMEM((dim, points), F32),
        pltpu.VMEM((points,), F32),
        pltpu.VMEM((probe_count, points), F32),
        pltpu.VMEM((probe_count, points), F32),
        pltpu.VMEM((1, dim), F32),
        pltpu.VMEM((8, 128), F32),
        pltpu.SemaphoreType.DMA((5,)),
        pltpu.SemaphoreType.DMA((SLOTS, chunks)),
        pltpu.SemaphoreType.DMA((SLOTS, chunks)),
    ]


def on_device(coords, alpha, probe_solves, probes, lengthscale):
    dim, points = coords.shape
    any_spec = pl.BlockSpec(memory_space=pl.ANY)
    vmem_spec = pl.BlockSpec(memory_space=pltpu.VMEM)
    return pl.pallas_call(
        functools.partial(kernel, lax.axis_size("blk")),
        out_shape=jax.ShapeDtypeStruct((dim, points), F32),
        in_specs=[any_spec] * 5,
        out_specs=vmem_spec,
        scratch_shapes=scratch_shapes(dim, points, probe_solves.shape[0]),
        compiler_params=pltpu.CompilerParams(collective_id=0, has_side_effects=True),
    )(coords, alpha, probe_solves, probes, lengthscale[None])


def solution(mesh):
    return jax.shard_map(
        on_device,
        mesh=mesh,
        in_specs=(
            P(None, ("groups", "blk")),
            P(("groups", "blk")),
            P(None, ("groups", "blk")),
            P(None, ("groups", "blk")),
            P(),
        ),
        out_specs=P(None, ("groups", "blk")),
        check_vma=False,
    )
```

```python
import functools
import math

import jax
import jax.numpy as jnp
from jax import lax
from jax.experimental import pallas as pl
from jax.experimental.pallas import tpu as pltpu
from jax.sharding import PartitionSpec as P

F32 = jnp.float32
BF16 = jnp.bfloat16
MESH = pl.DeviceIdType.MESH

UNIT = math.sqrt(5.0) * math.log2(math.e)
LN2 = math.log(2.0)

CHUNK = 256
DEPTH = 208
OWN, PARTNER, UP, DOWN, P_UP, P_DOWN, SLOTS = 0, 1, 2, 6, 10, 14, 18


def split3(x):
    hi = x.astype(BF16)
    rest = x - hi.astype(F32)
    mid = rest.astype(BF16)
    lo = (rest - mid.astype(F32)).astype(BF16)
    return hi, mid, lo


def split2(x):
    hi = x.astype(BF16)
    return hi, (x - hi.astype(F32)).astype(BF16)


def column_of(row, dim):
    sub = lax.broadcasted_iota(jnp.int32, (dim, dim), 0)
    lane = lax.broadcasted_iota(jnp.int32, (dim, dim), 1)
    full = jnp.broadcast_to(row, (dim, dim))
    return jnp.sum(jnp.where(sub == lane, full, 0.0), axis=1, keepdims=True)


def pick_rows(rows, shape):
    sub = lax.broadcasted_iota(jnp.int32, shape, 0)
    out = jnp.zeros(shape, F32)
    for index, value in enumerate(rows):
        out = jnp.where(sub == index, value, out)
    return out


def prepare(block, scale_ref, lhs_d, lhs_c, vis):
    scaled = block[0:32, :] * scale_ref[...]
    hi, mid, lo = split3(scaled)
    norm = [v.astype(F32) for v in split3(jnp.sum(scaled * scaled, 0, keepdims=True))]
    ends = pick_rows((1.0, 1.0, 1.0, *norm), (8, CHUNK))
    ends = jnp.concatenate([ends, jnp.zeros((8, CHUNK), F32)], 0).astype(BF16)
    rest = jnp.zeros((256 - DEPTH, CHUNK), BF16)
    lhs_d[...] = jnp.concatenate([hi, mid, lo, hi, mid, hi, ends, rest], 0).T
    t_hi, t_lo = split2(block[32:64, :])
    lhs_c[...] = jnp.concatenate([t_hi, t_lo, t_hi, t_lo], 0).T
    for side in (0, CHUNK):
        vis[0:32, side : side + CHUNK] = hi
        vis[32:64, side : side + CHUNK] = mid


def direct(lhs_d, lhs_c, rhs_d, rhs_c, w, lanes, floor_ref):
    floor = jnp.concatenate([jnp.concatenate([floor_ref[...]] * (CHUNK // 128), 1)] * 4, 0)
    dist = jnp.dot(lhs_d[:, 0:DEPTH], rhs_d[:, lanes], preferred_element_type=F32)
    coup = jnp.dot(lhs_c[...], rhs_c[:, lanes], preferred_element_type=F32)
    for start in range(0, CHUNK, 32):
        rows = slice(start, start + 32)
        d2 = jnp.maximum(dist[rows], floor)
        u = d2 * lax.rsqrt(d2)
        weight = (1.0 / LN2 + u) * jnp.exp2(-u) * coup[rows]
        w[rows, lanes] = weight.astype(BF16)
        lo = weight - w[rows, lanes].astype(F32)
        w[start + CHUNK : start + 32 + CHUNK, lanes] = lo.astype(BF16)


def gather_sums(vis, w, total, lanes):
    total[:, lanes] += jnp.dot(vis[...], w[:, lanes], preferred_element_type=F32)


def region(lhs_d, lhs_c, rhs_d, rhs_c, vis, vis_old, w, w_old, total, floor_ref, prep):
    if prep is not None:
        prep()
    for t in range(0, w.shape[1], CHUNK):
        lanes = slice(t, t + CHUNK)
        direct(lhs_d, lhs_c, rhs_d, rhs_c, w, lanes, floor_ref)
        gather_sums(vis_old, w_old, total, lanes)


def own_side(buf, scale_ref, rhs_d, rhs_c, chunks, probe_count):
    sub = lax.broadcasted_iota(jnp.int32, (32, CHUNK), 0)
    for q in range(chunks):
        lanes = slice(q * CHUNK, (q + 1) * CHUNK)
        block = buf[OWN, q]
        scaled = block[0:32, :] * scale_ref[...]
        hi, mid, lo = ((-2.0 * v.astype(F32)).astype(BF16) for v in split3(scaled))
        norm = [v.astype(F32) for v in split3(jnp.sum(scaled * scaled, 0, keepdims=True))]
        ends = pick_rows((*norm, 1.0, 1.0, 1.0), (16, CHUNK)).astype(BF16)
        rhs_d[:, lanes] = jnp.concatenate([hi, hi, hi, mid, mid, lo, ends], 0)
        swapped = jnp.concatenate([block[48:64, :], block[32:48, :]], 0)
        half_inv = LN2 / (2.0 * probe_count)
        table = jnp.where(
            sub == probe_count,
            LN2 * swapped,
            jnp.where(sub == 2 * probe_count + 1, 0.0, -half_inv * swapped),
        )
        t_hi, t_lo = split2(table)
        rhs_c[:, lanes] = jnp.concatenate([t_hi, t_hi, t_lo, t_lo], 0)


def kernel(size, coords_in, alpha_in, solves_in, probes_in, length_in, grad, *scratch):
    (buf, scale_ref, rhs_d, rhs_c, ld0, ld1, ld2, ld3, lc0, lc1, lc2, lc3, v0, v1, v2, v3,
     w0, w1, total, coords, alpha, solves, probes, length,
     floor_ref, out, in_sem, out_sem, send_sem, recv_sem) = scratch
    lhs_d, lhs_c, vis = (ld0, ld1, ld2, ld3), (lc0, lc1, lc2, lc3), (v0, v1, v2, v3)
    w = (w0, w1)
    dim, points = coords.shape
    probe_count = solves.shape[0]
    chunks = points // CHUNK
    hops = size // 8
    passes = hops * chunks

    group = lax.axis_index("groups")
    me = lax.axis_index("blk")
    core = lax.rem(me, 2)
    above = lax.rem(me + 2, size)
    below = lax.rem(me + size - 2, size)
    partner = me + 1 - 2 * core

    barrier = pltpu.get_barrier_semaphore()
    for other in (above, below, partner):
        pl.semaphore_signal(barrier, inc=1, device_id=(group, other), device_id_type=MESH)

    loads = [
        pltpu.make_async_copy(src, dst, in_sem.at[index])
        for index, (src, dst) in enumerate(
            ((coords_in, coords), (alpha_in, alpha), (solves_in, solves), (probes_in, probes),
             (length_in, length))
        )
    ]
    for load in loads:
        load.start()
    for load in loads:
        load.wait()

    for q in range(chunks):
        lanes = slice(q * CHUNK, (q + 1) * CHUNK)
        row = alpha[lanes].reshape(1, CHUNK)
        buf[OWN, q, 0:32, :] = coords[:, lanes]
        buf[OWN, q, 32:64, :] = jnp.concatenate(
            [solves[:, lanes], row, probes[:, lanes], row], 0
        )

    pl.semaphore_wait(barrier, 3)

    def send(src, dst, q, other):
        return pltpu.make_async_remote_copy(
            src_ref=buf.at[src, q],
            dst_ref=buf.at[dst, q],
            send_sem=send_sem.at[dst, q],
            recv_sem=recv_sem.at[dst, q],
            device_id=(group, other),
            device_id_type=MESH,
        )

    def arrived(slot, q):
        send(slot, slot, q, partner).wait_recv()

    for q in range(chunks):
        send(OWN, UP, q, above).start()
        send(OWN, DOWN, q, below).start()
        send(OWN, PARTNER, q, partner).start()

    give_src = jnp.where(core == 0, DOWN + hops - 1, UP + hops - 1)
    give_dst = jnp.where(core == 0, P_DOWN + hops - 1, P_UP + hops - 1)
    take = jnp.where(core == 0, P_UP + hops - 1, P_DOWN + hops - 1)

    def relay(k, last_hop):
        hop, q = k // chunks, lax.rem(k, chunks)
        arrived(UP + hop, q)
        arrived(DOWN + hop, q)
        if last_hop:
            send(give_src, give_dst, q, partner).start()
        else:
            send(UP + hop, UP + hop + 1, q, above).start()
            send(DOWN + hop, DOWN + hop + 1, q, below).start()
            send(UP + hop, P_UP + hop, q, partner).start()
            send(DOWN + hop, P_DOWN + hop, q, partner).start()

    def prep(slot, q, position):
        prepare(buf[slot, q], scale_ref, lhs_d[position], lhs_c[position], vis[position])

    def step(position, slot=None, q=None):
        here, there = position % 2, (position + 1) % 2
        ahead = None if slot is None else lambda: prep(slot, q, (position + 2) % 4)
        region(lhs_d[position], lhs_c[position], rhs_d, rhs_c, vis[position], vis[(position + 3) % 4],
               w[here], w[there], total, floor_ref, ahead)

    def up(k):
        return UP + k // chunks, lax.rem(k, chunks)

    def down(k):
        return DOWN + k // chunks, lax.rem(k, chunks)

    def side(k):
        return (P_UP + k // chunks, lax.rem(k, chunks)), (P_DOWN + k // chunks, lax.rem(k, chunks))

    inverse = 1.0 / column_of(length[...], dim)
    scale_ref[...] = jnp.broadcast_to(inverse * UNIT, (dim, CHUNK))
    own_side(buf, scale_ref, rhs_d, rhs_c, chunks, probe_count)
    total[...] = jnp.zeros_like(total)
    floor_ref[...] = jnp.full_like(floor_ref, 1e-30)
    w1[...] = jnp.zeros_like(w1)
    sub = lax.broadcasted_iota(jnp.int32, (16, 2 * CHUNK), 0)
    for v in vis:
        v[64:80, :] = jnp.where(sub == 0, 1.0, 0.0).astype(BF16)
    v3[0:64, :] = jnp.zeros((64, 2 * CHUNK), BF16)

    for q in range(chunks):
        arrived(PARTNER, q)
    prep(PARTNER, 0, 0)
    prep(PARTNER, 1, 1)
    step(0, PARTNER, 2)
    relay(0, False)
    step(1, UP, 0)
    step(2, DOWN, 0)
    step(3)
    step(0)
    relay(1, False)
    prep(UP, 1, 1)
    prep(DOWN, 1, 2)

    def turn(k, last_hop):
        left, right = side(k - 1)
        arrived(*left)
        arrived(*right)
        step(1, *left)
        step(2, *right)
        relay(k + 1, last_hop)
        step(3, *up(k + 1))
        step(0, *down(k + 1))

    @pl.loop(1, passes - chunks - 1)
    def _(k):
        turn(k, False)

    @pl.loop(passes - chunks - 1, passes - chunks + 1)
    def _(k):
        turn(k, True)

    arrived(take, 0)
    arrived(take, 1)
    step(1, take, 0)
    step(2, take, 1)
    relay(passes - 1, True)
    step(3, *up(passes - 1))
    step(0, *down(passes - 1))
    arrived(take, 2)
    step(1, take, 2)
    step(2)
    step(3)
    gather_sums(v3, w1, total, slice(0, points))

    for q in range(chunks):
        lanes = slice(q * CHUNK, (q + 1) * CHUNK)
        scaled = buf[OWN, q, 0:32, :] * scale_ref[...]
        summed = scaled * total[64:65, lanes] - (total[0:32, lanes] + total[32:64, lanes])
        out[:, lanes] = scale_ref[...] * (-5.0 / (3.0 * UNIT * UNIT)) * summed

    store = pltpu.make_async_copy(out, grad, out_sem)
    store.start()

    for q in range(chunks):
        send(OWN, PARTNER, q, partner).wait_send()
        for hop in range(hops):
            send(OWN, UP + hop, q, above).wait_send()
            send(OWN, DOWN + hop, q, below).wait_send()
            if hop < hops - 1:
                send(OWN, P_UP + hop, q, partner).wait_send()
                send(OWN, P_DOWN + hop, q, partner).wait_send()
        send(give_src, give_dst, q, partner).wait_send()
    store.wait()


def scratch_shapes(dim, points, probe_count):
    chunks = points // CHUNK
    return [
        pltpu.VMEM((SLOTS, chunks, 64, CHUNK), F32),
        pltpu.VMEM((dim, CHUNK), F32),
        pltpu.VMEM((DEPTH, points), BF16),
        pltpu.VMEM((128, points), BF16),
        *[pltpu.VMEM((CHUNK, 256), BF16)] * 4,
        *[pltpu.VMEM((CHUNK, 128), BF16)] * 4,
        *[pltpu.VMEM((80, 2 * CHUNK), BF16)] * 4,
        *[pltpu.VMEM((2 * CHUNK, points), BF16)] * 2,
        pltpu.VMEM((80, points), F32),
        pltpu.VMEM((dim, points), F32),
        pltpu.VMEM((points,), F32),
        pltpu.VMEM((probe_count, points), F32),
        pltpu.VMEM((probe_count, points), F32),
        pltpu.VMEM((1, dim), F32),
        pltpu.VMEM((8, 128), F32),
        pltpu.VMEM((dim, points), F32),
        pltpu.SemaphoreType.DMA((5,)),
        pltpu.SemaphoreType.DMA,
        pltpu.SemaphoreType.DMA((SLOTS, chunks)),
        pltpu.SemaphoreType.DMA((SLOTS, chunks)),
    ]


def on_device(coords, alpha, probe_solves, probes, lengthscale):
    dim, points = coords.shape
    any_spec = pl.BlockSpec(memory_space=pl.ANY)
    return pl.pallas_call(
        functools.partial(kernel, lax.axis_size("blk")),
        out_shape=jax.ShapeDtypeStruct((dim, points), F32),
        in_specs=[any_spec] * 5,
        out_specs=any_spec,
        scratch_shapes=scratch_shapes(dim, points, probe_solves.shape[0]),
        compiler_params=pltpu.CompilerParams(collective_id=0, has_side_effects=True),
    )(coords, alpha, probe_solves, probes, lengthscale[None])


def solution(mesh):
    return jax.shard_map(
        on_device,
        mesh=mesh,
        in_specs=(
            P(None, ("groups", "blk")),
            P(("groups", "blk")),
            P(None, ("groups", "blk")),
            P(None, ("groups", "blk")),
            P(),
        ),
        out_specs=P(None, ("groups", "blk")),
        check_vma=False,
    )
```

```python
import functools
import math

import jax
import jax.numpy as jnp
from jax import lax
from jax.experimental import pallas as pl
from jax.experimental.pallas import tpu as pltpu
from jax.sharding import PartitionSpec as P

F32 = jnp.float32
BF16 = jnp.bfloat16
MESH = pl.DeviceIdType.MESH

UNIT = math.sqrt(5.0) * math.log2(math.e)
LN2 = math.log(2.0)

CHUNK = 256
DEPTH = 208
OWN, PARTNER, UP, DOWN, P_UP, P_DOWN, SLOTS = 0, 1, 2, 6, 10, 14, 18


def split3(x):
    hi = x.astype(BF16)
    rest = x - hi.astype(F32)
    mid = rest.astype(BF16)
    lo = (rest - mid.astype(F32)).astype(BF16)
    return hi, mid, lo


def split2(x):
    hi = x.astype(BF16)
    return hi, (x - hi.astype(F32)).astype(BF16)


def column_of(row, dim):
    sub = lax.broadcasted_iota(jnp.int32, (dim, dim), 0)
    lane = lax.broadcasted_iota(jnp.int32, (dim, dim), 1)
    full = jnp.broadcast_to(row, (dim, dim))
    return jnp.sum(jnp.where(sub == lane, full, 0.0), axis=1, keepdims=True)


def pick_rows(rows, shape):
    sub = lax.broadcasted_iota(jnp.int32, shape, 0)
    out = jnp.zeros(shape, F32)
    for index, value in enumerate(rows):
        out = jnp.where(sub == index, value, out)
    return out


def prepare(block, scale_ref, lhs_d, lhs_c, vis):
    scaled = block[0:32, :] * scale_ref[...]
    hi, mid, lo = split3(scaled)
    norm = [v.astype(F32) for v in split3(jnp.sum(scaled * scaled, 0, keepdims=True))]
    ends = pick_rows((1.0, 1.0, 1.0, *norm), (8, CHUNK))
    ends = jnp.concatenate([ends, jnp.zeros((8, CHUNK), F32)], 0).astype(BF16)
    rest = jnp.zeros((256 - DEPTH, CHUNK), BF16)
    lhs_d[...] = jnp.concatenate([hi, mid, lo, hi, mid, hi, ends, rest], 0).T
    t_hi, t_lo = split2(block[32:64, :])
    lhs_c[...] = jnp.concatenate([t_hi, t_lo, t_hi, t_lo], 0).T
    for side in (0, CHUNK):
        vis[0:32, side : side + CHUNK] = hi
        vis[32:64, side : side + CHUNK] = mid


def direct(lhs_d, lhs_c, rhs_d, rhs_c, w, lanes, floor_ref):
    floor = jnp.concatenate([jnp.concatenate([floor_ref[...]] * (CHUNK // 128), 1)] * 4, 0)
    dist = jnp.dot(lhs_d[:, 0:DEPTH], rhs_d[:, lanes], preferred_element_type=F32)
    coup = jnp.dot(lhs_c[...], rhs_c[:, lanes], preferred_element_type=F32)
    for start in range(0, CHUNK, 32):
        rows = slice(start, start + 32)
        d2 = jnp.maximum(dist[rows], floor)
        u = d2 * lax.rsqrt(d2)
        weight = (1.0 / LN2 + u) * jnp.exp2(-u) * coup[rows]
        w[rows, lanes] = weight.astype(BF16)
        lo = weight - w[rows, lanes].astype(F32)
        w[start + CHUNK : start + 32 + CHUNK, lanes] = lo.astype(BF16)


def gather_sums(vis, w, total, lanes):
    total[:, lanes] += jnp.dot(vis[...], w[:, lanes], preferred_element_type=F32)


def region(lhs_d, lhs_c, rhs_d, rhs_c, vis, vis_old, w, w_old, total, floor_ref, prep):
    if prep is not None:
        prep()
    for t in range(0, w.shape[1], CHUNK):
        lanes = slice(t, t + CHUNK)
        direct(lhs_d, lhs_c, rhs_d, rhs_c, w, lanes, floor_ref)
        gather_sums(vis_old, w_old, total, lanes)


def own_side(buf, scale_ref, rhs_d, rhs_c, chunks, probe_count):
    sub = lax.broadcasted_iota(jnp.int32, (32, CHUNK), 0)
    for q in range(chunks):
        lanes = slice(q * CHUNK, (q + 1) * CHUNK)
        block = buf[OWN, q]
        scaled = block[0:32, :] * scale_ref[...]
        hi, mid, lo = ((-2.0 * v.astype(F32)).astype(BF16) for v in split3(scaled))
        norm = [v.astype(F32) for v in split3(jnp.sum(scaled * scaled, 0, keepdims=True))]
        ends = pick_rows((*norm, 1.0, 1.0, 1.0), (16, CHUNK)).astype(BF16)
        rhs_d[:, lanes] = jnp.concatenate([hi, hi, hi, mid, mid, lo, ends], 0)
        swapped = jnp.concatenate([block[48:64, :], block[32:48, :]], 0)
        half_inv = LN2 / (2.0 * probe_count)
        table = jnp.where(
            sub == probe_count,
            LN2 * swapped,
            jnp.where(sub == 2 * probe_count + 1, 0.0, -half_inv * swapped),
        )
        t_hi, t_lo = split2(table)
        rhs_c[:, lanes] = jnp.concatenate([t_hi, t_hi, t_lo, t_lo], 0)


def kernel(size, coords_in, alpha_in, solves_in, probes_in, length_in, grad, *scratch):
    (buf, scale_ref, rhs_d, rhs_c, ld0, ld1, ld2, ld3, lc0, lc1, lc2, lc3, v0, v1, v2, v3,
     w0, w1, total, coords, alpha, solves, probes, length,
     floor_ref, out, in_sem, out_sem, send_sem, recv_sem) = scratch
    lhs_d, lhs_c, vis = (ld0, ld1, ld2, ld3), (lc0, lc1, lc2, lc3), (v0, v1, v2, v3)
    w = (w0, w1)
    dim, points = coords.shape
    probe_count = solves.shape[0]
    chunks = points // CHUNK
    hops = size // 8
    passes = hops * chunks

    group = lax.axis_index("groups")
    me = lax.axis_index("blk")
    core = lax.rem(me, 2)
    above = lax.rem(me + 2, size)
    below = lax.rem(me + size - 2, size)
    partner = me + 1 - 2 * core

    barrier = pltpu.get_barrier_semaphore()
    for other in (above, below, partner):
        pl.semaphore_signal(barrier, inc=1, device_id=(group, other), device_id_type=MESH)

    loads = [
        pltpu.make_async_copy(src, dst, in_sem.at[index])
        for index, (src, dst) in enumerate(
            ((coords_in, coords), (alpha_in, alpha), (solves_in, solves), (probes_in, probes),
             (length_in, length))
        )
    ]
    for load in loads:
        load.start()
    for load in loads:
        load.wait()

    for q in range(chunks):
        lanes = slice(q * CHUNK, (q + 1) * CHUNK)
        row = alpha[lanes].reshape(1, CHUNK)
        buf[OWN, q, 0:32, :] = coords[:, lanes]
        buf[OWN, q, 32:64, :] = jnp.concatenate(
            [solves[:, lanes], row, probes[:, lanes], row], 0
        )

    pl.semaphore_wait(barrier, 3)

    def send(src, dst, q, other):
        return pltpu.make_async_remote_copy(
            src_ref=buf.at[src, q],
            dst_ref=buf.at[dst, q],
            send_sem=send_sem.at[dst, q],
            recv_sem=recv_sem.at[dst, q],
            device_id=(group, other),
            device_id_type=MESH,
        )

    def arrived(slot, q):
        send(slot, slot, q, partner).wait_recv()

    for q in range(chunks):
        send(OWN, UP, q, above).start()
        send(OWN, DOWN, q, below).start()
        send(OWN, PARTNER, q, partner).start()

    give_src = jnp.where(core == 0, DOWN + hops - 1, UP + hops - 1)
    give_dst = jnp.where(core == 0, P_DOWN + hops - 1, P_UP + hops - 1)
    take = jnp.where(core == 0, P_UP + hops - 1, P_DOWN + hops - 1)

    def relay(k, last_hop):
        hop, q = k // chunks, lax.rem(k, chunks)
        arrived(UP + hop, q)
        arrived(DOWN + hop, q)
        if last_hop:
            send(give_src, give_dst, q, partner).start()
        else:
            send(UP + hop, UP + hop + 1, q, above).start()
            send(DOWN + hop, DOWN + hop + 1, q, below).start()
            send(UP + hop, P_UP + hop, q, partner).start()
            send(DOWN + hop, P_DOWN + hop, q, partner).start()

    def prep(slot, q, position):
        prepare(buf[slot, q], scale_ref, lhs_d[position], lhs_c[position], vis[position])

    def step(position, slot=None, q=None):
        here, there = position % 2, (position + 1) % 2
        ahead = None if slot is None else lambda: prep(slot, q, (position + 2) % 4)
        region(lhs_d[position], lhs_c[position], rhs_d, rhs_c, vis[position], vis[(position + 3) % 4],
               w[here], w[there], total, floor_ref, ahead)

    def up(k):
        return UP + k // chunks, lax.rem(k, chunks)

    def down(k):
        return DOWN + k // chunks, lax.rem(k, chunks)

    def side(k):
        return (P_UP + k // chunks, lax.rem(k, chunks)), (P_DOWN + k // chunks, lax.rem(k, chunks))

    inverse = 1.0 / column_of(length[...], dim)
    scale_ref[...] = jnp.broadcast_to(inverse * UNIT, (dim, CHUNK))
    own_side(buf, scale_ref, rhs_d, rhs_c, chunks, probe_count)
    total[...] = jnp.zeros_like(total)
    floor_ref[...] = jnp.full_like(floor_ref, 1e-30)
    w1[...] = jnp.zeros_like(w1)
    sub = lax.broadcasted_iota(jnp.int32, (16, 2 * CHUNK), 0)
    for v in vis:
        v[64:80, :] = jnp.where(sub == 0, 1.0, 0.0).astype(BF16)
    v3[0:64, :] = jnp.zeros((64, 2 * CHUNK), BF16)

    for q in range(chunks):
        arrived(PARTNER, q)
    prep(PARTNER, 0, 0)
    prep(PARTNER, 1, 1)
    step(0, PARTNER, 2)
    step(1)
    step(2)
    relay(0, False)
    prep(UP, 0, 3)
    prep(DOWN, 0, 0)
    step(3)
    step(0)
    relay(1, False)
    prep(UP, 1, 1)
    prep(DOWN, 1, 2)

    def turn(k, last_hop):
        left, right = side(k - 1)
        arrived(*left)
        arrived(*right)
        step(1, *left)
        step(2, *right)
        relay(k + 1, last_hop)
        step(3, *up(k + 1))
        step(0, *down(k + 1))

    @pl.loop(1, passes - chunks - 1)
    def _(k):
        turn(k, False)

    @pl.loop(passes - chunks - 1, passes - chunks + 1)
    def _(k):
        turn(k, True)

    arrived(take, 0)
    arrived(take, 1)
    step(1, take, 0)
    step(2, take, 1)
    relay(passes - 1, True)
    step(3, *up(passes - 1))
    step(0, *down(passes - 1))
    arrived(take, 2)
    step(1, take, 2)
    step(2)
    step(3)
    gather_sums(v3, w1, total, slice(0, points))

    for q in range(chunks):
        lanes = slice(q * CHUNK, (q + 1) * CHUNK)
        scaled = buf[OWN, q, 0:32, :] * scale_ref[...]
        summed = scaled * total[64:65, lanes] - (total[0:32, lanes] + total[32:64, lanes])
        out[:, lanes] = scale_ref[...] * (-5.0 / (3.0 * UNIT * UNIT)) * summed

    store = pltpu.make_async_copy(out, grad, out_sem)
    store.start()

    for q in range(chunks):
        send(OWN, PARTNER, q, partner).wait_send()
        for hop in range(hops):
            send(OWN, UP + hop, q, above).wait_send()
            send(OWN, DOWN + hop, q, below).wait_send()
            if hop < hops - 1:
                send(OWN, P_UP + hop, q, partner).wait_send()
                send(OWN, P_DOWN + hop, q, partner).wait_send()
        send(give_src, give_dst, q, partner).wait_send()
    store.wait()


def scratch_shapes(dim, points, probe_count):
    chunks = points // CHUNK
    return [
        pltpu.VMEM((SLOTS, chunks, 64, CHUNK), F32),
        pltpu.VMEM((dim, CHUNK), F32),
        pltpu.VMEM((DEPTH, points), BF16),
        pltpu.VMEM((128, points), BF16),
        *[pltpu.VMEM((CHUNK, 256), BF16)] * 4,
        *[pltpu.VMEM((CHUNK, 128), BF16)] * 4,
        *[pltpu.VMEM((80, 2 * CHUNK), BF16)] * 4,
        *[pltpu.VMEM((2 * CHUNK, points), BF16)] * 2,
        pltpu.VMEM((80, points), F32),
        pltpu.VMEM((dim, points), F32),
        pltpu.VMEM((points,), F32),
        pltpu.VMEM((probe_count, points), F32),
        pltpu.VMEM((probe_count, points), F32),
        pltpu.VMEM((1, dim), F32),
        pltpu.VMEM((8, 128), F32),
        pltpu.VMEM((dim, points), F32),
        pltpu.SemaphoreType.DMA((5,)),
        pltpu.SemaphoreType.DMA,
        pltpu.SemaphoreType.DMA((SLOTS, chunks)),
        pltpu.SemaphoreType.DMA((SLOTS, chunks)),
    ]


def on_device(coords, alpha, probe_solves, probes, lengthscale):
    dim, points = coords.shape
    any_spec = pl.BlockSpec(memory_space=pl.ANY)
    return pl.pallas_call(
        functools.partial(kernel, lax.axis_size("blk")),
        out_shape=jax.ShapeDtypeStruct((dim, points), F32),
        in_specs=[any_spec] * 5,
        out_specs=any_spec,
        scratch_shapes=scratch_shapes(dim, points, probe_solves.shape[0]),
        compiler_params=pltpu.CompilerParams(collective_id=0,
            has_side_effects=True,),
    )(coords, alpha, probe_solves, probes, lengthscale[None])


def solution(mesh):
    return jax.shard_map(
        on_device,
        mesh=mesh,
        in_specs=(
            P(None, ("groups", "blk")),
            P(("groups", "blk")),
            P(None, ("groups", "blk")),
            P(None, ("groups", "blk")),
            P(),
        ),
        out_specs=P(None, ("groups", "blk")),
        check_vma=False,
    )
```

```python
import functools
import math

import jax
import jax.numpy as jnp
from jax import lax
from jax.experimental import pallas as pl
from jax.experimental.pallas import tpu as pltpu
from jax.sharding import PartitionSpec as P

F32 = jnp.float32
BF16 = jnp.bfloat16
MESH = pl.DeviceIdType.MESH

UNIT = math.sqrt(5.0) * math.log2(math.e)
LN2 = math.log(2.0)

CHUNK = 256
DEPTH = 208
OWN, PARTNER, UP, DOWN, P_UP, P_DOWN, SLOTS = 0, 1, 2, 6, 10, 14, 18


def split3(x):
    hi = x.astype(BF16)
    rest = x - hi.astype(F32)
    mid = rest.astype(BF16)
    lo = (rest - mid.astype(F32)).astype(BF16)
    return hi, mid, lo


def split2(x):
    hi = x.astype(BF16)
    return hi, (x - hi.astype(F32)).astype(BF16)


def column_of(row, dim):
    sub = lax.broadcasted_iota(jnp.int32, (dim, dim), 0)
    lane = lax.broadcasted_iota(jnp.int32, (dim, dim), 1)
    full = jnp.broadcast_to(row, (dim, dim))
    return jnp.sum(jnp.where(sub == lane, full, 0.0), axis=1, keepdims=True)


def pick_rows(rows, shape):
    sub = lax.broadcasted_iota(jnp.int32, shape, 0)
    out = jnp.zeros(shape, F32)
    for index, value in enumerate(rows):
        out = jnp.where(sub == index, value, out)
    return out


def prepare(block, scale_ref, lhs_d, lhs_c, vis):
    scaled = block[0:32, :] * scale_ref[...]
    hi, mid, lo = split3(scaled)
    norm = [v.astype(F32) for v in split3(jnp.sum(scaled * scaled, 0, keepdims=True))]
    ends = pick_rows((1.0, 1.0, 1.0, *norm), (8, CHUNK))
    ends = jnp.concatenate([ends, jnp.zeros((8, CHUNK), F32)], 0).astype(BF16)
    rest = jnp.zeros((256 - DEPTH, CHUNK), BF16)
    lhs_d[...] = jnp.concatenate([hi, mid, lo, hi, mid, hi, ends, rest], 0).T
    t_hi, t_lo = split2(block[32:64, :])
    lhs_c[...] = jnp.concatenate([t_hi, t_lo, t_hi, t_lo], 0).T
    for side in (0, CHUNK):
        vis[0:32, side : side + CHUNK] = hi
        vis[32:64, side : side + CHUNK] = mid


def direct(lhs_d, lhs_c, rhs_d, rhs_c, w, lanes, floor_ref):
    floor = jnp.concatenate([jnp.concatenate([floor_ref[...]] * (CHUNK // 128), 1)] * 4, 0)
    dist = jnp.dot(lhs_d[:, 0:DEPTH], rhs_d[:, lanes], preferred_element_type=F32)
    coup = jnp.dot(lhs_c[...], rhs_c[:, lanes], preferred_element_type=F32)
    for start in range(0, CHUNK, 32):
        rows = slice(start, start + 32)
        d2 = jnp.maximum(dist[rows], floor)
        u = d2 * lax.rsqrt(d2)
        weight = (1.0 / LN2 + u) * jnp.exp2(-u) * coup[rows]
        w[rows, lanes] = weight.astype(BF16)
        lo = weight - w[rows, lanes].astype(F32)
        w[start + CHUNK : start + 32 + CHUNK, lanes] = lo.astype(BF16)


def gather_sums(vis, w, total, lanes):
    total[:, lanes] += jnp.dot(vis[...], w[:, lanes], preferred_element_type=F32)


def region(lhs_d, lhs_c, rhs_d, rhs_c, vis, vis_old, w, w_old, total, floor_ref, prep):
    if prep is not None:
        prep()
    for t in range(0, w.shape[1], CHUNK):
        lanes = slice(t, t + CHUNK)
        direct(lhs_d, lhs_c, rhs_d, rhs_c, w, lanes, floor_ref)
        gather_sums(vis_old, w_old, total, lanes)


def own_side(buf, scale_ref, rhs_d, rhs_c, chunks, probe_count):
    sub = lax.broadcasted_iota(jnp.int32, (32, CHUNK), 0)
    for q in range(chunks):
        lanes = slice(q * CHUNK, (q + 1) * CHUNK)
        block = buf[OWN, q]
        scaled = block[0:32, :] * scale_ref[...]
        hi, mid, lo = ((-2.0 * v.astype(F32)).astype(BF16) for v in split3(scaled))
        norm = [v.astype(F32) for v in split3(jnp.sum(scaled * scaled, 0, keepdims=True))]
        ends = pick_rows((*norm, 1.0, 1.0, 1.0), (16, CHUNK)).astype(BF16)
        rhs_d[:, lanes] = jnp.concatenate([hi, hi, hi, mid, mid, lo, ends], 0)
        swapped = jnp.concatenate([block[48:64, :], block[32:48, :]], 0)
        half_inv = LN2 / (2.0 * probe_count)
        table = jnp.where(
            sub == probe_count,
            LN2 * swapped,
            jnp.where(sub == 2 * probe_count + 1, 0.0, -half_inv * swapped),
        )
        t_hi, t_lo = split2(table)
        rhs_c[:, lanes] = jnp.concatenate([t_hi, t_hi, t_lo, t_lo], 0)


def kernel(size, coords_in, alpha_in, solves_in, probes_in, length_in, grad, *scratch):
    (buf, scale_ref, rhs_d, rhs_c, ld0, ld1, ld2, ld3, lc0, lc1, lc2, lc3, v0, v1, v2, v3,
     w0, w1, total, coords, alpha, solves, probes, length,
     floor_ref, out, in_sem, out_sem, send_sem, recv_sem) = scratch
    lhs_d, lhs_c, vis = (ld0, ld1, ld2, ld3), (lc0, lc1, lc2, lc3), (v0, v1, v2, v3)
    w = (w0, w1)
    dim, points = coords.shape
    probe_count = solves.shape[0]
    chunks = points // CHUNK
    hops = size // 8
    passes = hops * chunks

    group = lax.axis_index("groups")
    me = lax.axis_index("blk")
    core = lax.rem(me, 2)
    above = lax.rem(me + 2, size)
    below = lax.rem(me + size - 2, size)
    partner = me + 1 - 2 * core

    barrier = pltpu.get_barrier_semaphore()
    for other in (above, below, partner):
        pl.semaphore_signal(barrier, inc=1, device_id=(group, other), device_id_type=MESH)

    loads = [
        pltpu.make_async_copy(src, dst, in_sem.at[index])
        for index, (src, dst) in enumerate(
            ((coords_in, coords), (alpha_in, alpha), (solves_in, solves), (probes_in, probes),
             (length_in, length))
        )
    ]
    for load in loads:
        load.start()
    for load in loads:
        load.wait()

    for q in range(chunks):
        lanes = slice(q * CHUNK, (q + 1) * CHUNK)
        row = alpha[lanes].reshape(1, CHUNK)
        buf[OWN, q, 0:32, :] = coords[:, lanes]
        buf[OWN, q, 32:64, :] = jnp.concatenate(
            [solves[:, lanes], row, probes[:, lanes], row], 0
        )

    pl.semaphore_wait(barrier, 3)

    def send(src, dst, q, other):
        return pltpu.make_async_remote_copy(
            src_ref=buf.at[src, q],
            dst_ref=buf.at[dst, q],
            send_sem=send_sem.at[dst, q],
            recv_sem=recv_sem.at[dst, q],
            device_id=(group, other),
            device_id_type=MESH,
        )

    def arrived(slot, q):
        send(slot, slot, q, partner).wait_recv()

    for q in range(chunks):
        send(OWN, UP, q, above).start()
        send(OWN, DOWN, q, below).start()
        send(OWN, PARTNER, q, partner).start()

    give_src = jnp.where(core == 0, DOWN + hops - 1, UP + hops - 1)
    give_dst = jnp.where(core == 0, P_DOWN + hops - 1, P_UP + hops - 1)
    take = jnp.where(core == 0, P_UP + hops - 1, P_DOWN + hops - 1)

    def relay(k, last_hop):
        hop, q = k // chunks, lax.rem(k, chunks)
        arrived(UP + hop, q)
        arrived(DOWN + hop, q)
        if last_hop:
            send(give_src, give_dst, q, partner).start()
        else:
            send(UP + hop, UP + hop + 1, q, above).start()
            send(DOWN + hop, DOWN + hop + 1, q, below).start()
            send(UP + hop, P_UP + hop, q, partner).start()
            send(DOWN + hop, P_DOWN + hop, q, partner).start()

    def prep(slot, q, position):
        prepare(buf[slot, q], scale_ref, lhs_d[position], lhs_c[position], vis[position])

    def step(position, slot=None, q=None):
        here, there = position % 2, (position + 1) % 2
        ahead = None if slot is None else lambda: prep(slot, q, (position + 2) % 4)
        region(lhs_d[position], lhs_c[position], rhs_d, rhs_c, vis[position], vis[(position + 3) % 4],
               w[here], w[there], total, floor_ref, ahead)

    def up(k):
        return UP + k // chunks, lax.rem(k, chunks)

    def down(k):
        return DOWN + k // chunks, lax.rem(k, chunks)

    def side(k):
        return (P_UP + k // chunks, lax.rem(k, chunks)), (P_DOWN + k // chunks, lax.rem(k, chunks))

    inverse = 1.0 / column_of(length[...], dim)
    scale_ref[...] = jnp.broadcast_to(inverse * UNIT, (dim, CHUNK))
    own_side(buf, scale_ref, rhs_d, rhs_c, chunks, probe_count)
    total[...] = jnp.zeros_like(total)
    floor_ref[...] = jnp.full_like(floor_ref, 1e-30)
    w1[...] = jnp.zeros_like(w1)
    sub = lax.broadcasted_iota(jnp.int32, (16, 2 * CHUNK), 0)
    for v in vis:
        v[64:80, :] = jnp.where(sub == 0, 1.0, 0.0).astype(BF16)
    v3[0:64, :] = jnp.zeros((64, 2 * CHUNK), BF16)

    for q in range(chunks):
        arrived(PARTNER, q)
    prep(PARTNER, 0, 0)
    prep(PARTNER, 1, 1)
    step(0, PARTNER, 2)
    step(1)
    step(2)
    relay(0, False)
    prep(UP, 0, 3)
    prep(DOWN, 0, 0)
    step(3)
    step(0)
    relay(1, False)
    prep(UP, 1, 1)
    prep(DOWN, 1, 2)

    def turn(k, last_hop):
        left, right = side(k - 1)
        arrived(*left)
        arrived(*right)
        step(1, *left)
        step(2, *right)
        relay(k + 1, last_hop)
        step(3, *up(k + 1))
        step(0, *down(k + 1))

    @pl.loop(1, passes - chunks - 1)
    def _(k):
        turn(k, False)

    @pl.loop(passes - chunks - 1, passes - chunks + 1)
    def _(k):
        turn(k, True)

    arrived(take, 0)
    relay(passes - 1, True)
    step(1, take, 0)
    step(2, *up(passes - 1))
    step(3, *down(passes - 1))
    arrived(take, 1)
    arrived(take, 2)
    step(0, take, 1)
    step(1, take, 2)
    step(2)
    step(3)
    gather_sums(v3, w1, total, slice(0, points))

    for q in range(chunks):
        lanes = slice(q * CHUNK, (q + 1) * CHUNK)
        scaled = buf[OWN, q, 0:32, :] * scale_ref[...]
        summed = scaled * total[64:65, lanes] - (total[0:32, lanes] + total[32:64, lanes])
        out[:, lanes] = scale_ref[...] * (-5.0 / (3.0 * UNIT * UNIT)) * summed

    store = pltpu.make_async_copy(out, grad, out_sem)
    store.start()

    for q in range(chunks):
        send(OWN, PARTNER, q, partner).wait_send()
        for hop in range(hops):
            send(OWN, UP + hop, q, above).wait_send()
            send(OWN, DOWN + hop, q, below).wait_send()
            if hop < hops - 1:
                send(OWN, P_UP + hop, q, partner).wait_send()
                send(OWN, P_DOWN + hop, q, partner).wait_send()
        send(give_src, give_dst, q, partner).wait_send()
    store.wait()


def scratch_shapes(dim, points, probe_count):
    chunks = points // CHUNK
    return [
        pltpu.VMEM((SLOTS, chunks, 64, CHUNK), F32),
        pltpu.VMEM((dim, CHUNK), F32),
        pltpu.VMEM((DEPTH, points), BF16),
        pltpu.VMEM((128, points), BF16),
        *[pltpu.VMEM((CHUNK, 256), BF16)] * 4,
        *[pltpu.VMEM((CHUNK, 128), BF16)] * 4,
        *[pltpu.VMEM((80, 2 * CHUNK), BF16)] * 4,
        *[pltpu.VMEM((2 * CHUNK, points), BF16)] * 2,
        pltpu.VMEM((80, points), F32),
        pltpu.VMEM((dim, points), F32),
        pltpu.VMEM((points,), F32),
        pltpu.VMEM((probe_count, points), F32),
        pltpu.VMEM((probe_count, points), F32),
        pltpu.VMEM((1, dim), F32),
        pltpu.VMEM((8, 128), F32),
        pltpu.VMEM((dim, points), F32),
        pltpu.SemaphoreType.DMA((5,)),
        pltpu.SemaphoreType.DMA,
        pltpu.SemaphoreType.DMA((SLOTS, chunks)),
        pltpu.SemaphoreType.DMA((SLOTS, chunks)),
    ]


def on_device(coords, alpha, probe_solves, probes, lengthscale):
    dim, points = coords.shape
    any_spec = pl.BlockSpec(memory_space=pl.ANY)
    return pl.pallas_call(
        functools.partial(kernel, lax.axis_size("blk")),
        out_shape=jax.ShapeDtypeStruct((dim, points), F32),
        in_specs=[any_spec] * 5,
        out_specs=any_spec,
        scratch_shapes=scratch_shapes(dim, points, probe_solves.shape[0]),
        compiler_params=pltpu.CompilerParams(
            collective_id=0,
            has_side_effects=True,
        ),
    )(coords, alpha, probe_solves, probes, lengthscale[None])


def solution(mesh):
    return jax.shard_map(
        on_device,
        mesh=mesh,
        in_specs=(
            P(None, ("groups", "blk")),
            P(("groups", "blk")),
            P(None, ("groups", "blk")),
            P(None, ("groups", "blk")),
            P(),
        ),
        out_specs=P(None, ("groups", "blk")),
        check_vma=False,
    )
```
